32 devices in a mesh: seq: 8 (over z, x), head: 4 (over y, core).
Axes of the slice: x: 2, y: 2, z: 4, core: 2. Of those that a mesh axis runs over, the one named last changes fastest.
Arguments:
- queries: bfloat16 [2048, 2048], P('seq', 'head'), may hold values from -8 to 8
- keys: bfloat16 [2048, 512], P('seq', 'head'), may hold values from -4 to 4
- values: bfloat16 [2048, 512], P('seq', 'head'), may hold values from -6 to 6
- doc_ids: int32 [2048], replicated, may hold values from 0 to 15, never falling along the last dimension, each value on 1 to 1024 neighbouring positions
- span_order: int32 [16], replicated, may hold values from 0 to 15, each once
- out_weight: bfloat16 [2048, 4096], P('head', 'seq'), may hold values from -0.1875 to 0.1875
Outputs:
- layer_out: bfloat16 [2048, 4096], P('seq', 'head')
The draws below stay inside these ranges and needn't reach their ends.
All inputs are finite; a program needn't handle non-finite values.
Results may differ from the reference program's by a relative error of at most 0.012.
Values may be sent and summed in bfloat16 or wider, within the bound.
A program may use at most 64 MiB of HBM per device.

```python
import math
import jax
import jax.numpy as jnp
import numpy as np
from jax import lax

D = 4096
HEADS = 16
KV_HEADS = 4
DH = 128
GROUP = 4
TOK_DEV = 256
SEQ = 2048
DOCS = 16
MAX_DOC = 1024
N_SEQ = 8


def draw_queries(key, part):
    base = jnp.clip(jax.random.normal(jax.random.fold_in(key, 11), (SEQ, HEADS * DH), jnp.float32), -4.0, 4.0)
    return base.astype(jnp.bfloat16)


def draw_keys(key, part):
    base = jnp.clip(jax.random.normal(jax.random.fold_in(key, 21), (SEQ, KV_HEADS * DH), jnp.float32), -4.0, 4.0)
    return base.astype(jnp.bfloat16)


def spiked(result, key, source, target, parts, factor):
    owner, partner = [(jnp.arange(result.shape[dim]) // (result.shape[dim] // parts)).reshape([-1 if axis == dim else 1 for axis in range(result.ndim)]) for dim in (source, target)]
    chosen = jax.random.permutation(key, parts)[partner]
    strong = (owner == chosen) | (owner == (partner + parts // 2) % parts)
    return jnp.where(strong, factor * result, result)


def block_scale(own_key, shape, pieces, least, high):
    def one(axis_at, shards_of):
        steps = jax.random.uniform(jax.random.fold_in(jax.random.fold_in(own_key, 6), axis_at), (shards_of,), jnp.float32, least / len(pieces), high / len(pieces))
        return jnp.repeat(jnp.exp(steps), shape[axis_at] // shards_of).reshape((-1,) + (1,) * (len(shape) - axis_at - 1))

    level = one(*pieces[0])
    for cut in pieces[1:]:
        level = level * one(*cut)
    return level


def length_profile(amount, total, limit, lean):
    loads = [(1 << 20) // math.isqrt(grade ** lean) + 1 for grade in range(2, amount + 1)]
    surplus, given = total - limit - (amount - 1), [1] * (amount - 1)
    while surplus > 0:
        candidates = [i for i in range(amount - 1) if given[i] < limit]
        whole, remaining = sum([loads[i] for i in candidates]), surplus
        for i in candidates:
            more = min(limit - given[i], max(1, remaining * loads[i] // whole), surplus)
            given[i] = given[i] + more
            surplus = surplus - more
    return np.array([limit] + given)


def ragged_sizes(stream_key, amount, total, most, lean):
    if amount == 2:
        one = jax.random.randint(stream_key, (), max(1, total - most), min(most, total - 1) + 1)
        return jnp.stack([one, total - one])
    tallies = jnp.asarray(length_profile(amount, total, most, lean), jnp.int32)
    pairs = (amount - 1) // 2
    donor, taker = tallies[1:1 + 2 * pairs:2], tallies[2:2 + 2 * pairs:2]
    slack = jnp.minimum(donor - 1, most - taker)
    shifted = jax.random.randint(jax.random.fold_in(stream_key, 1), (pairs,), 0, 1 << 20) % (slack + 1)
    tallies = tallies.at[1:1 + 2 * pairs:2].set(donor - shifted).at[2:2 + 2 * pairs:2].set(taker + shifted)
    return tallies[jax.random.permutation(jax.random.fold_in(stream_key, 2), amount)]


def centred(rng, dims, width, bound, cuts=(), kind=jnp.bfloat16):
    entries = jax.random.normal(rng, dims, jnp.float32) * width
    if len(cuts) > 0:
        entries = block_scale(rng, dims, cuts, -0.22, 0.18) * entries
    return jnp.clip(entries, min=-bound, max=bound).astype(kind)


def noise_with(own_key, shape, spread, reach, split, heavy, kind=jnp.bfloat16):
    values = spread * jax.random.normal(own_key, shape, jnp.float32)
    if split:
        values = values * block_scale(own_key, shape, split, -0.22, 0.18)
    return jnp.clip(spiked(values, jax.random.fold_in(own_key, 3), *heavy), -reach, reach).astype(kind)


def setup_inputs(seed: int = 0) -> dict:
    arg_keys = jax.random.split(jax.random.key(seed), 7)
    return {
        "queries": draw_queries(jax.random.fold_in(arg_keys[6], 71), 0),
        "keys": draw_keys(jax.random.fold_in(arg_keys[6], 71), 0),
        "values": centred(arg_keys[2], (SEQ, KV_HEADS * DH), 1.0, 6.0, ((0, 8), (1, 4))),
        "doc_ids": jnp.searchsorted(jnp.cumsum(ragged_sizes(arg_keys[3], DOCS, SEQ, MAX_DOC, 2)), jnp.arange(SEQ), side="right").astype(jnp.int32),
        "span_order": jax.random.permutation(arg_keys[4], 2 * N_SEQ).astype(jnp.int32),
        "out_weight": noise_with(arg_keys[5], (HEADS * DH, D), (HEADS * DH) ** -0.5, 0.1875, ((0, 4), (1, 8)), (0, 1, 8, 2.0)),
    }


def reference(queries, keys, values, doc_ids, span_order, out_weight):
    span = TOK_DEV // 2
    rows = jnp.arange(SEQ, dtype=jnp.int32)
    pos = (span_order[rows // span] * span + rows % span).astype(jnp.int32)
    doc = doc_ids[pos]
    scale = 1.0 / math.sqrt(DH)
    key_all = keys.reshape(SEQ, KV_HEADS, DH).astype(jnp.float32)
    val_all = values.reshape(SEQ, KV_HEADS, DH).astype(jnp.float32)
    block = math.gcd(SEQ, 128)

    def one_block(index):
        start = (index * block).astype(jnp.int32)
        qblk = lax.dynamic_slice_in_dim(queries, start, block, 0)
        qblk = qblk.reshape(block, KV_HEADS, GROUP, DH).astype(jnp.float32)
        qpos = lax.dynamic_slice_in_dim(pos, start, block, 0)
        qdoc = lax.dynamic_slice_in_dim(doc, start, block, 0)
        scores = jnp.einsum('qhgd,khd->hgqk', qblk, key_all) * scale
        visible = (qdoc[:, None] == doc[None, :]) & (pos[None, :] <= qpos[:, None])
        masked = jnp.where(visible, scores, jnp.float32(-1e+30))
        largest = lax.optimization_barrier(jnp.max(masked, axis=-1, keepdims=True))
        weights = jnp.where(visible, jnp.exp(masked - largest), jnp.float32(0.0))
        total = lax.optimization_barrier(jnp.sum(weights, axis=-1))
        weights_b = weights.astype(jnp.bfloat16).astype(jnp.float32)
        summed = jnp.einsum('hgqk,khd->qhgd', weights_b, val_all)
        attended = summed / jnp.transpose(total, (2, 0, 1))[..., None]
        return attended.astype(jnp.bfloat16).reshape(block, HEADS * DH)
    attended = lax.map(one_block, jnp.arange(SEQ // block, dtype=jnp.int32))
    attended = attended.reshape(SEQ, HEADS * DH)
    return jnp.dot(attended, out_weight, preferred_element_type=jnp.float32).astype(jnp.bfloat16)
```

```python
import functools
import math

import jax
import jax.numpy as jnp
from jax import lax
from jax.experimental import pallas as pl
from jax.experimental.pallas import tpu as pltpu
from jax.sharding import PartitionSpec as P

MESH = pl.DeviceIdType.MESH

DH = 128
NEG = -1e30

def gathered_form(queries, keys, values, doc_ids, span_order, out_weight):
    tok_rows = queries.shape[0]
    span = tok_rows // 2
    local_heads = queries.shape[1] // DH
    local_kv = keys.shape[1] // DH
    group_size = local_heads // local_kv
    n_blocks = span_order.shape[0]
    scale = 1.0 / math.sqrt(DH)
    mine = lax.axis_index("seq")
    own_blocks = lax.dynamic_slice_in_dim(span_order, 2 * mine, 2, 0)
    local_rows = jnp.arange(tok_rows, dtype=jnp.int32)
    qpos = jnp.where(local_rows < span, own_blocks[0], own_blocks[1]) * span + local_rows % span
    qdoc = jnp.take(doc_ids, qpos)
    q_heads = queries.reshape(tok_rows, local_kv, group_size, DH)

    def update(state, kblk, vblk, kpos, kdoc):
        largest, total, summed = state
        count = kblk.shape[0]
        k_heads = kblk.reshape(count, local_kv, DH)
        v_heads = vblk.reshape(count, local_kv, DH)
        scores = (
            jnp.einsum("qhgd,khd->hgqk", q_heads, k_heads, preferred_element_type=jnp.float32)
            * scale
        )
        visible = (qdoc[:, None] == kdoc[None, :]) & (kpos[None, :] <= qpos[:, None])
        masked = jnp.where(visible, scores, jnp.float32(-1e30))
        new_largest = jnp.maximum(largest, jnp.max(masked, axis=-1))
        factor = jnp.exp(largest - new_largest)
        weights = jnp.where(visible, jnp.exp(masked - new_largest[..., None]), jnp.float32(0.0))
        total = total * factor + jnp.sum(weights, axis=-1)
        weights_b = weights.astype(jnp.bfloat16)
        added = jnp.einsum("hgqk,khd->qhgd", weights_b, v_heads, preferred_element_type=jnp.float32)
        summed = summed * jnp.transpose(factor, (2, 0, 1))[..., None] + added
        return (new_largest, total, summed)

    initial = (
        jnp.full((local_kv, group_size, tok_rows), -1e30, jnp.float32),
        jnp.zeros((local_kv, group_size, tok_rows), jnp.float32),
        jnp.zeros((tok_rows, local_kv, group_size, DH), jnp.float32),
    )
    state = initial
    kpiece = lax.all_gather(keys, "seq", axis=0, tiled=True)
    vpiece = lax.all_gather(values, "seq", axis=0, tiled=True)
    count = kpiece.shape[0]
    width = math.gcd(count, 1024)
    steps = count // width
    rows = jnp.arange(count, dtype=jnp.int32)
    match = (rows // span)[:, None] == jnp.arange(n_blocks, dtype=jnp.int32)[None, :]
    owner = jnp.sum(jnp.where(match, span_order[None, :], 0), axis=1)
    kpos = owner * span + rows % span
    kdoc = jnp.take(doc_ids, kpos)
    kparts = kpiece.reshape(steps, width, kpiece.shape[1])
    vparts = vpiece.reshape(steps, width, vpiece.shape[1])

    def one_step(carry, items):
        kblk, vblk, pblk, dblk = items
        carry = update(carry, kblk, vblk, pblk, dblk)
        return (carry, None)

    state, unused = lax.scan(
        one_step, state, (kparts, vparts, kpos.reshape(steps, width), kdoc.reshape(steps, width))
    )
    largest, total, summed = state
    attended = (summed / jnp.transpose(total, (2, 0, 1))[..., None]).astype(jnp.bfloat16)
    attended = attended.reshape(tok_rows, local_heads * DH)
    partial_out = jnp.dot(
        attended,
        lax.all_gather(out_weight, "seq", axis=1, tiled=True),
        preferred_element_type=jnp.float32,
    )
    return lax.psum_scatter(
        partial_out.astype(jnp.bfloat16), "head", scatter_dimension=1, tiled=True
    )


def line_kernel(
    n, q_in, k_in, v_in, doc_in, order_in, w_in, out_ref,
    q_ref, doc_ref, order_ref, fetched, kbuf, vbuf, wbuf, bias, best, acc, att, far, stage, sums,
    kv_send, kv_recv, w_send, w_recv, att_send, att_recv, far_send, far_recv, sum_send, sum_recv,
):
    seq, head = lax.axis_index("seq"), lax.axis_index("head")
    z, x, y, c = seq // 2, seq % 2, head // 2, head % 2
    side = z // 2
    role = (z + side) % 2
    rows = q_ref.shape[0]
    span = rows // 2
    heads = q_ref.shape[1] // DH
    depth, width = w_in.shape
    half, deep = width // 2, depth // 2
    factor = math.log2(math.e) / math.sqrt(DH)
    slabs = n // 2
    far_slab = slabs - 1
    cuts = range(2)
    parts = [(cut, low) for cut in range(2) for low in range(2)]

    def slab(k):
        return k + side * (slabs - 1 - 2 * k)

    def place(zz, xx, yy, cc):
        return {"seq": 2 * zz + xx, "head": 2 * yy + cc}

    inward = place((1 - role) * slab(1) + role * slab(2), x, y, c)
    outward = place(slab(0), x, y, c)
    across = {"seq": 2 * z + 1 - x}
    partner = {"head": 2 * y + 1 - c}
    ways = (inward, outward, across)

    own = role
    fetches = [
        pltpu.make_async_copy(src, dst, fetched.at[at])
        for at, (src, dst) in enumerate(
            [(k_in, kbuf.at[own, 0]), (v_in, vbuf.at[own, 0])]
            + [
                (w_in.at[pl.ds(low * deep, deep), pl.ds(cut * half, half)], wbuf.at[own, cut, pl.ds(low * deep, deep)])
                for cut, low in parts
            ]
            + [(doc_in, doc_ref), (order_in, order_ref), (q_in, q_ref)]
        )
    ]
    for fetch in fetches:
        fetch.start()

    barrier = pltpu.get_barrier_semaphore()
    for zz in range(2):
        for flip in range(8):
            fx, fy, fc = flip // 4, flip // 2 % 2, flip % 2
            if zz or flip:
                there = place((z - 2 * side + zz) % 2 + 2 * side, (x + fx) % 2, (y + fy) % 2, (c + fc) % 2)
                pl.semaphore_signal(barrier, inc=1, device_id=there, device_id_type=MESH)

    @pl.when(role == 1)
    def _():
        pl.semaphore_signal(barrier, inc=1, device_id=inward, device_id_type=MESH)

    pl.semaphore_wait(barrier, 15 + role)

    def remote(src, dst, send, recv, device):
        return pltpu.make_async_remote_copy(
            src_ref=src, dst_ref=dst, send_sem=send, recv_sem=recv, device_id=device, device_id_type=MESH
        )

    sent = ([], [])

    def go(who, make):
        make().start()
        sent[who].append(make)

    def arrive(dst, recv):
        remote(dst, dst, att_send.at[0], recv, partner).wait_recv()

    def kv_send_to(who, which, way, k):
        buf = (kbuf, vbuf)[which]
        to = slabs - 1 - k if (who == 1 and way == 0) else k
        lane = 1 if way == 2 else 0
        go(
            who,
            lambda: remote(
                buf.at[k, 0], buf.at[to, lane], kv_send.at[which, way, k], kv_recv.at[which, lane, to], ways[way]
            ),
        )

    def kv_wait(which, lane, k):
        arrive((kbuf, vbuf)[which].at[k, lane], kv_recv.at[which, lane, k])

    def w_at(k, cut, low, mine):
        return wbuf.at[k, cut, pl.ds(mine * depth + low * deep, deep)]

    def w_send_to(who, way, k, cut, low):
        to = slabs - 1 - k if (who == 1 and way == 0) else k
        mine = 1 if way == 2 else 0
        go(
            who,
            lambda: remote(
                w_at(k, cut, low, 0), w_at(to, cut, low, mine), w_send.at[way, k, cut, low],
                w_recv.at[mine, to, cut, low], partner if way == 2 else ways[way],
            ),
        )

    def w_wait(mine, k, cut, low):
        arrive(w_at(k, cut, low, mine), w_recv.at[mine, k, cut, low])

    def each(end, middle):
        @pl.when(role == 0)
        def _():
            end(0)

        @pl.when(role == 1)
        def _():
            middle(1)

    for which in range(2):
        fetches[which].wait()

        def end(who):
            for way in (0, 2):
                kv_send_to(who, which, way, 0)

        def middle(who):
            for way in (1, 0, 2):
                kv_send_to(who, which, way, 1)

        each(end, middle)
    for fetch in fetches[2:]:
        fetch.wait()

    def end(who):
        for cut, low in parts:
            w_send_to(who, 0, 0, cut, low)
        for cut, low in parts:
            w_send_to(who, 2, 0, cut, low)

    def middle(who):
        for cut, low in parts:
            w_send_to(who, 2, 1, cut, low)

    each(end, middle)

    down = lax.broadcasted_iota(jnp.int32, (span, span), 0)
    along = lax.broadcasted_iota(jnp.int32, (span, span), 1)
    query_at, query_doc = [], []
    for part in range(2):
        block = order_ref[2 * seq + part]
        query_at.append(down + block * span)
        docs = doc_ref[pl.ds(block, 1), :].astype(jnp.float32)
        query_doc.append(jnp.transpose(jnp.broadcast_to(docs, (span, span))))

    order = (role, 1 - role, 2, 3)

    def mask(step):
        for lane in range(2):
            source = 2 * slab(order[step]) + (x if lane == 0 else 1 - x)
            for j in range(2):
                block = order_ref[2 * source + j]
                docs = doc_ref[pl.ds(block, 1), :].astype(jnp.float32)
                key_at = along + block * span
                first = (2 * lane + j) * span
                for part in range(2):
                    seen = (query_doc[part] == docs) & (key_at <= query_at[part])
                    bias[step % 2, part * span : (part + 1) * span, first : first + span] = jnp.where(
                        seen, jnp.float32(0.0), jnp.float32(NEG)
                    )

    def attend(step, h):
        k = order[step]
        count = 2 * rows
        q = q_ref[:, h * DH : (h + 1) * DH]
        scores = lax.dot_general(
            q, kbuf[k].reshape(count, DH), (((1,), (1,)), ((), ())), preferred_element_type=jnp.float32
        )
        masked = scores * factor + bias[step % 2]
        top = jnp.broadcast_to(jnp.max(masked, axis=-1, keepdims=True), (rows, DH))
        if step > 0:
            before = best[h]
            top = jnp.maximum(before, top)
        weights = jnp.concatenate(
            [jnp.exp2(masked[:, at : at + DH] - top).astype(jnp.bfloat16) for at in range(0, count, DH)], axis=1
        )
        wide = jnp.concatenate([vbuf[k].reshape(count, DH), jnp.ones((count, DH), jnp.bfloat16)], axis=1)
        summed = jnp.dot(weights, wide, preferred_element_type=jnp.float32)
        if step > 0:
            fade = jnp.exp2(before - top)
            summed = summed + acc[h] * jnp.concatenate([fade, fade], axis=1)
        if step < slabs - 1:
            best[h] = top
            acc[h] = summed
        else:
            att[2, :, h * DH : (h + 1) * DH] = (summed[:, :DH] / summed[:, DH:]).astype(jnp.bfloat16)

    def group(step):
        for which in range(2):
            kv_wait(which, 1, order[step])
        for h in range(heads):
            attend(step, h)

    mask(0)

    def end(who):
        for which in range(2):
            kv_wait(which, 0, 1)
            kv_send_to(who, which, 2, 1)

    def middle(who):
        for which in range(2):
            kv_wait(which, 0, 0)
            kv_send_to(who, which, 0, 0)
            kv_send_to(who, which, 2, 0)
            kv_wait(which, 0, 2)
            kv_send_to(who, which, 1, 2)
            kv_send_to(who, which, 2, 2)
        for cut, low in parts:
            w_send_to(who, 0, 1, cut, low)

    each(end, middle)
    mask(1)
    group(0)

    def end(who):
        for which in range(2):
            kv_wait(which, 0, 2)
            kv_send_to(who, which, 2, 2)

    def middle(who):
        for which in range(2):
            kv_wait(which, 0, 3)
            kv_send_to(who, which, 1, 3)
            kv_send_to(who, which, 2, 3)
        for cut, low in parts:
            w_send_to(who, 1, 1, cut, low)

    each(end, middle)
    group(1)
    mask(2)
    mask(3)

    def end(who):
        for which in range(2):
            kv_wait(which, 0, 3)
            kv_send_to(who, which, 2, 3)

    each(end, lambda who: None)
    group(2)
    group(3)

    cross = place(z, 1 - x, y, x)
    own_rows = c == x
    cross_part = (c + x) % 2
    first_part = 2 * (1 - cross_part)

    def att_cross():
        return remote(att.at[2], att.at[cross_part], att_send.at[0], att_recv.at[cross_part], cross)

    def att_near():
        return remote(att.at[2], att.at[1], att_send.at[1], att_recv.at[1], partner)

    att_cross().start()

    @pl.when(jnp.logical_not(own_rows))
    def _():
        att_near().start()

    def pass_w(who, k, which, way):
        for cut, low in which:
            w_wait(0, k, cut, low)
            if way is not None:
                w_send_to(who, way, k, cut, low)
            w_send_to(who, 2, k, cut, low)

    def att_wait():
        arrive(att.at[1], att_recv.at[1])

        @pl.when(jnp.logical_not(own_rows))
        def _():
            arrive(att.at[0], att_recv.at[0])

    def end(who):
        pass_w(who, 1, parts[:2], None)

    def middle(who):
        pass_w(who, 0, parts[:2], 0)
        pass_w(who, 2, parts[:1], 1)
        pass_w(who, 0, parts[2:], 0)
        pass_w(who, 2, parts[1:], 1)

    each(end, middle)
    att_wait()

    def far_copy(part):
        src = first_part if part == 0 else 1
        return remote(att.at[src], far.at[part], far_send.at[part], far_recv.at[part], inward)

    def end(who):
        for part in range(2):
            go(who, functools.partial(far_copy, part))

    each(end, lambda who: None)

    def sum_copy(k, slot, cut, zz):
        return remote(
            stage.at[slot, cut], sums.at[y, x, cut], sum_send.at[slot, cut], sum_recv.at[y, x, cut],
            {"seq": 2 * zz + c, "head": slab(k)},
        )

    def here(k):
        return own_rows & (slab(k) == head)

    def product(k, cut, first, second):
        added = jnp.dot(first, wbuf[k, cut, :depth, :], preferred_element_type=jnp.float32)
        return added + jnp.dot(second, wbuf[k, cut, depth:, :], preferred_element_type=jnp.float32)

    def project(k, slot, cut):
        value = product(k, cut, att[first_part], att[1]).astype(jnp.bfloat16)

        @pl.when(here(k))
        def _():
            sums[y, x, cut] = value

        @pl.when(jnp.logical_not(here(k)))
        def _():
            stage[slot, cut] = value
            sum_copy(k, slot, cut, z).start()

    def project_far(who, cut):
        stage[slabs, cut] = product(far_slab, cut, far[0], far[1]).astype(jnp.bfloat16)
        go(who, lambda: sum_copy(far_slab, slabs, cut, slab(0)))

    def near_w(k, cut):
        for low in range(2):
            w_wait(1, k, cut, low)

    for cut in cuts:
        near_w(order[0], cut)
        project(order[0], 0, cut)

    def end(who):
        pass_w(who, 1, parts[2:], None)

    each(end, lambda who: None)
    for cut in cuts:
        near_w(order[1], cut)
        project(order[1], 1, cut)
    for cut in cuts:

        def end(who):
            pass_w(who, 2, [(cut, low) for low in range(2)], None)

        each(end, lambda who: None)
        near_w(2, cut)
        project(2, 2, cut)

    def middle(who):
        for cut in cuts:
            pass_w(who, 3, [(cut, low) for low in range(2)], None)
            near_w(3, cut)
            if cut == 0:
                for part in range(2):
                    arrive(far.at[part], far_recv.at[part])
            project_far(who, cut)
            project(3, 3, cut)

    each(lambda who: None, middle)

    stays = own_rows & ((role == 1) | (slab(far_slab) != head))
    for cut in cuts:
        for lane in range(2):
            for row in range(2):

                @pl.when(jnp.logical_not(stays & (row == y) & (lane == x)))
                def _():
                    arrive(sums.at[row, lane, cut], sum_recv.at[row, lane, cut])

            at = lane * width + cut * half
            out_ref[:, at : at + half] = (
                sums[0, lane, cut].astype(jnp.float32) + sums[1, lane, cut].astype(jnp.float32)
            ).astype(jnp.bfloat16)

    def finish(who):
        for make in sent[who]:
            make().wait_send()

    each(finish, finish)
    att_cross().wait_send()

    @pl.when(jnp.logical_not(own_rows))
    def _():
        att_near().wait_send()

    for step in range(slabs):
        k = order[step]
        made = jnp.logical_not(here(k))
        if step == far_slab:
            made = made & (role == 1)

        @pl.when(made)
        def _(k=k, step=step):
            for cut in cuts:
                sum_copy(k, step, cut, z).wait_send()


def line_form(n, queries, keys, values, doc_ids, span_order, out_weight):
    rows = queries.shape[0]
    depth, width = out_weight.shape
    half = width // 2
    slabs = n // 2
    heads = queries.shape[1] // DH
    bf16 = jnp.bfloat16
    dma = pltpu.SemaphoreType.DMA
    return pl.pallas_call(
        functools.partial(line_kernel, n),
        out_shape=jax.ShapeDtypeStruct((rows, 2 * width), bf16),
        in_specs=[pl.BlockSpec(memory_space=pl.ANY)] * 6,
        out_specs=pl.BlockSpec(memory_space=pltpu.VMEM),
        scratch_shapes=[
            pltpu.VMEM(queries.shape, bf16),
            pltpu.VMEM((doc_ids.shape[0] // (rows // 2), rows // 2), jnp.int32),
            pltpu.SMEM(span_order.shape, jnp.int32),
            dma((9,)),
            pltpu.VMEM((slabs, 2, rows, DH), bf16),
            pltpu.VMEM((slabs, 2, rows, DH), bf16),
            pltpu.VMEM((slabs, 2, 2 * depth, half), bf16),
            pltpu.VMEM((2, rows, 2 * rows), jnp.float32),
            pltpu.VMEM((heads, rows, DH), jnp.float32),
            pltpu.VMEM((heads, rows, 2 * DH), jnp.float32),
            pltpu.VMEM((3,) + queries.shape, bf16),
            pltpu.VMEM((2,) + queries.shape, bf16),
            pltpu.VMEM((slabs + 1, 2, rows, half), bf16),
            pltpu.VMEM((2, 2, 2, rows, half), bf16),
            dma((2, 3, slabs)),
            dma((2, 2, slabs)),
            dma((3, slabs, 2, 2)),
            dma((2, slabs, 2, 2)),
            dma((2,)),
            dma((2,)),
            dma((2,)),
            dma((2,)),
            dma((slabs + 1, 2)),
            dma((2, 2, 2)),
        ],
        compiler_params=pltpu.CompilerParams(
            collective_id=0, has_side_effects=True, vmem_limit_bytes=62 * 1024 * 1024
        ),
    )(queries, keys, values, doc_ids.reshape(-1, rows // 2), span_order, out_weight)


def on_device(mesh_shape, queries, keys, values, doc_ids, span_order, out_weight):
    n, groups = mesh_shape["seq"], mesh_shape["head"]
    rows = queries.shape[0]
    depth, width = out_weight.shape
    fits = (
        groups == 4
        and n == 2 * groups
        and rows == 2 * DH
        and keys.shape[1] == DH
        and queries.shape[1] == depth
        and depth % (2 * DH) == 0
        and width % (4 * DH) == 0
        and depth * width <= 512 * 512
    )
    if fits:
        return line_form(n, queries, keys, values, doc_ids, span_order, out_weight)
    return gathered_form(queries, keys, values, doc_ids, span_order, out_weight)


def solution(mesh):
    return jax.shard_map(
        functools.partial(on_device, dict(mesh.shape)),
        mesh=mesh,
        in_specs=(P("seq", "head"), P("seq", "head"), P("seq", "head"), P(), P(), P("head", "seq")),
        out_specs=P("seq", "head"),
        check_vma=False,
    )
```

```python
import functools
import math

import jax
import jax.numpy as jnp
from jax import lax
from jax.experimental import pallas as pl
from jax.experimental.pallas import tpu as pltpu
from jax.sharding import PartitionSpec as P

MESH = pl.DeviceIdType.MESH

DH = 128
NEG = -1e30

def gathered_form(queries, keys, values, doc_ids, span_order, out_weight):
    tok_rows = queries.shape[0]
    span = tok_rows // 2
    local_heads = queries.shape[1] // DH
    local_kv = keys.shape[1] // DH
    group_size = local_heads // local_kv
    n_blocks = span_order.shape[0]
    scale = 1.0 / math.sqrt(DH)
    mine = lax.axis_index("seq")
    own_blocks = lax.dynamic_slice_in_dim(span_order, 2 * mine, 2, 0)
    local_rows = jnp.arange(tok_rows, dtype=jnp.int32)
    qpos = jnp.where(local_rows < span, own_blocks[0], own_blocks[1]) * span + local_rows % span
    qdoc = jnp.take(doc_ids, qpos)
    q_heads = queries.reshape(tok_rows, local_kv, group_size, DH)

    def update(state, kblk, vblk, kpos, kdoc):
        largest, total, summed = state
        count = kblk.shape[0]
        k_heads = kblk.reshape(count, local_kv, DH)
        v_heads = vblk.reshape(count, local_kv, DH)
        scores = (
            jnp.einsum("qhgd,khd->hgqk", q_heads, k_heads, preferred_element_type=jnp.float32)
            * scale
        )
        visible = (qdoc[:, None] == kdoc[None, :]) & (kpos[None, :] <= qpos[:, None])
        masked = jnp.where(visible, scores, jnp.float32(-1e30))
        new_largest = jnp.maximum(largest, jnp.max(masked, axis=-1))
        factor = jnp.exp(largest - new_largest)
        weights = jnp.where(visible, jnp.exp(masked - new_largest[..., None]), jnp.float32(0.0))
        total = total * factor + jnp.sum(weights, axis=-1)
        weights_b = weights.astype(jnp.bfloat16)
        added = jnp.einsum("hgqk,khd->qhgd", weights_b, v_heads, preferred_element_type=jnp.float32)
        summed = summed * jnp.transpose(factor, (2, 0, 1))[..., None] + added
        return (new_largest, total, summed)

    initial = (
        jnp.full((local_kv, group_size, tok_rows), -1e30, jnp.float32),
        jnp.zeros((local_kv, group_size, tok_rows), jnp.float32),
        jnp.zeros((tok_rows, local_kv, group_size, DH), jnp.float32),
    )
    state = initial
    kpiece = lax.all_gather(keys, "seq", axis=0, tiled=True)
    vpiece = lax.all_gather(values, "seq", axis=0, tiled=True)
    count = kpiece.shape[0]
    width = math.gcd(count, 1024)
    steps = count // width
    rows = jnp.arange(count, dtype=jnp.int32)
    match = (rows // span)[:, None] == jnp.arange(n_blocks, dtype=jnp.int32)[None, :]
    owner = jnp.sum(jnp.where(match, span_order[None, :], 0), axis=1)
    kpos = owner * span + rows % span
    kdoc = jnp.take(doc_ids, kpos)
    kparts = kpiece.reshape(steps, width, kpiece.shape[1])
    vparts = vpiece.reshape(steps, width, vpiece.shape[1])

    def one_step(carry, items):
        kblk, vblk, pblk, dblk = items
        carry = update(carry, kblk, vblk, pblk, dblk)
        return (carry, None)

    state, unused = lax.scan(
        one_step, state, (kparts, vparts, kpos.reshape(steps, width), kdoc.reshape(steps, width))
    )
    largest, total, summed = state
    attended = (summed / jnp.transpose(total, (2, 0, 1))[..., None]).astype(jnp.bfloat16)
    attended = attended.reshape(tok_rows, local_heads * DH)
    partial_out = jnp.dot(
        attended,
        lax.all_gather(out_weight, "seq", axis=1, tiled=True),
        preferred_element_type=jnp.float32,
    )
    return lax.psum_scatter(
        partial_out.astype(jnp.bfloat16), "head", scatter_dimension=1, tiled=True
    )


def line_kernel(
    n, q_in, k_in, v_in, doc_in, order_in, w_in, out_ref,
    q_ref, doc_ref, order_ref, fetched, kbuf, vbuf, wbuf, bias, best, acc, att, far, stage, sums,
    kv_send, kv_recv, w_send, w_recv, att_send, att_recv, far_send, far_recv, sum_send, sum_recv,
):
    seq, head = lax.axis_index("seq"), lax.axis_index("head")
    z, x, y, c = seq // 2, seq % 2, head // 2, head % 2
    side = z // 2
    role = (z + side) % 2
    rows = q_ref.shape[0]
    span = rows // 2
    heads = q_ref.shape[1] // DH
    depth, width = w_in.shape
    half, deep = width // 2, depth // 2
    factor = math.log2(math.e) / math.sqrt(DH)
    slabs = n // 2
    far_slab = slabs - 1
    cuts = range(2)
    parts = [(cut, low) for cut in range(2) for low in range(2)]

    def slab(k):
        return k + side * (slabs - 1 - 2 * k)

    def place(zz, xx, yy, cc):
        return {"seq": 2 * zz + xx, "head": 2 * yy + cc}

    inward = place((1 - role) * slab(1) + role * slab(2), x, y, c)
    outward = place(slab(0), x, y, c)
    across = {"seq": 2 * z + 1 - x}
    partner = {"head": 2 * y + 1 - c}
    ways = (inward, outward, across)

    own = role
    fetches = [
        pltpu.make_async_copy(src, dst, fetched.at[at])
        for at, (src, dst) in enumerate(
            [(k_in, kbuf.at[own, 0]), (v_in, vbuf.at[own, 0])]
            + [
                (w_in.at[pl.ds(low * deep, deep), pl.ds(cut * half, half)], wbuf.at[own, cut, pl.ds(low * deep, deep)])
                for cut, low in parts
            ]
            + [(doc_in, doc_ref), (order_in, order_ref), (q_in, q_ref)]
        )
    ]
    for fetch in fetches:
        fetch.start()

    barrier = pltpu.get_barrier_semaphore()
    for zz in range(2):
        for flip in range(8):
            fx, fy, fc = flip // 4, flip // 2 % 2, flip % 2
            if zz or flip:
                there = place((z - 2 * side + zz) % 2 + 2 * side, (x + fx) % 2, (y + fy) % 2, (c + fc) % 2)
                pl.semaphore_signal(barrier, inc=1, device_id=there, device_id_type=MESH)

    @pl.when(role == 1)
    def _():
        pl.semaphore_signal(barrier, inc=1, device_id=inward, device_id_type=MESH)

    pl.semaphore_wait(barrier, 15 + role)

    def remote(src, dst, send, recv, device):
        return pltpu.make_async_remote_copy(
            src_ref=src, dst_ref=dst, send_sem=send, recv_sem=recv, device_id=device, device_id_type=MESH
        )

    sent = ([], [])

    def go(who, make):
        make().start()
        sent[who].append(make)

    def arrive(dst, recv):
        remote(dst, dst, att_send.at[0], recv, partner).wait_recv()

    def kv_send_to(who, which, way, k):
        buf = (kbuf, vbuf)[which]
        to = slabs - 1 - k if (who == 1 and way == 0) else k
        lane = 1 if way == 2 else 0
        go(
            who,
            lambda: remote(
                buf.at[k, 0], buf.at[to, lane], kv_send.at[which, way, k], kv_recv.at[which, lane, to], ways[way]
            ),
        )

    def kv_wait(which, lane, k):
        arrive((kbuf, vbuf)[which].at[k, lane], kv_recv.at[which, lane, k])

    def w_at(k, cut, low, mine):
        return wbuf.at[k, cut, pl.ds(mine * depth + low * deep, deep)]

    def w_send_to(who, way, k, cut, low):
        to = slabs - 1 - k if (who == 1 and way == 0) else k
        mine = 1 if way == 2 else 0
        go(
            who,
            lambda: remote(
                w_at(k, cut, low, 0), w_at(to, cut, low, mine), w_send.at[way, k, cut, low],
                w_recv.at[mine, to, cut, low], partner if way == 2 else ways[way],
            ),
        )

    def w_wait(mine, k, cut, low):
        arrive(w_at(k, cut, low, mine), w_recv.at[mine, k, cut, low])

    def each(end, middle):
        @pl.when(role == 0)
        def _():
            end(0)

        @pl.when(role == 1)
        def _():
            middle(1)

    for which in range(2):
        fetches[which].wait()

        def end(who):
            for way in (0, 2):
                kv_send_to(who, which, way, 0)

        def middle(who):
            for way in (1, 0, 2):
                kv_send_to(who, which, way, 1)

        each(end, middle)
    for fetch in fetches[2:]:
        fetch.wait()


    down = lax.broadcasted_iota(jnp.int32, (span, span), 0)
    along = lax.broadcasted_iota(jnp.int32, (span, span), 1)
    query_at, query_doc = [], []
    for part in range(2):
        block = order_ref[2 * seq + part]
        query_at.append(down + block * span)
        docs = doc_ref[pl.ds(block, 1), :].astype(jnp.float32)
        query_doc.append(jnp.transpose(jnp.broadcast_to(docs, (span, span))))

    order = (role, 1 - role, 2, 3)

    def mask(step):
        for lane in range(2):
            source = 2 * slab(order[step]) + (x if lane == 0 else 1 - x)
            for j in range(2):
                block = order_ref[2 * source + j]
                docs = doc_ref[pl.ds(block, 1), :].astype(jnp.float32)
                key_at = along + block * span
                first = (2 * lane + j) * span
                for part in range(2):
                    seen = (query_doc[part] == docs) & (key_at <= query_at[part])
                    bias[step % 2, part * span : (part + 1) * span, first : first + span] = jnp.where(
                        seen, jnp.float32(0.0), jnp.float32(NEG)
                    )

    def attend(step, h):
        k = order[step]
        count = 2 * rows
        q = q_ref[:, h * DH : (h + 1) * DH]
        scores = lax.dot_general(
            q, kbuf[k].reshape(count, DH), (((1,), (1,)), ((), ())), preferred_element_type=jnp.float32
        )
        masked = scores * factor + bias[step % 2]
        top = jnp.broadcast_to(jnp.max(masked, axis=-1, keepdims=True), (rows, DH))
        if step > 0:
            before = best[h]
            top = jnp.maximum(before, top)
        weights = jnp.concatenate(
            [jnp.exp2(masked[:, at : at + DH] - top).astype(jnp.bfloat16) for at in range(0, count, DH)], axis=1
        )
        wide = jnp.concatenate([vbuf[k].reshape(count, DH), jnp.ones((count, DH), jnp.bfloat16)], axis=1)
        summed = jnp.dot(weights, wide, preferred_element_type=jnp.float32)
        if step > 0:
            fade = jnp.exp2(before - top)
            summed = summed + acc[h] * jnp.concatenate([fade, fade], axis=1)
        if step < slabs - 1:
            best[h] = top
            acc[h] = summed
        else:
            att[2, :, h * DH : (h + 1) * DH] = (summed[:, :DH] / summed[:, DH:]).astype(jnp.bfloat16)

    def group(step):
        for which in range(2):
            kv_wait(which, 1, order[step])
        for h in range(heads):
            attend(step, h)

    mask(0)

    def end(who):
        for which in range(2):
            kv_wait(which, 0, 1)
            kv_send_to(who, which, 2, 1)
        for cut, low in parts:
            w_send_to(who, 0, 0, cut, low)
        for cut, low in parts:
            w_send_to(who, 2, 0, cut, low)

    def middle(who):
        for which in range(2):
            kv_wait(which, 0, 0)
            kv_send_to(who, which, 0, 0)
            kv_send_to(who, which, 2, 0)
            kv_wait(which, 0, 2)
            kv_send_to(who, which, 1, 2)
            kv_send_to(who, which, 2, 2)
        for cut, low in parts:
            w_send_to(who, 0, 1, cut, low)
        for which in range(2):
            kv_wait(which, 0, 3)
            kv_send_to(who, which, 1, 3)
            kv_send_to(who, which, 2, 3)
        for cut, low in parts[:2]:
            w_send_to(who, 1, 1, cut, low)
        for cut, low in parts:
            w_send_to(who, 2, 1, cut, low)

    each(end, middle)
    mask(1)
    group(0)

    def end(who):
        for which in range(2):
            kv_wait(which, 0, 2)
            kv_send_to(who, which, 2, 2)

    each(end, lambda who: None)
    group(1)
    mask(2)
    mask(3)

    def pass_w(who, k, which, way):
        for cut, low in which:
            w_wait(0, k, cut, low)
            if way is not None:
                w_send_to(who, way, k, cut, low)
            w_send_to(who, 2, k, cut, low)

    def end(who):
        for which in range(2):
            kv_wait(which, 0, 3)
            kv_send_to(who, which, 2, 3)

    def middle(who):
        pass_w(who, 2, parts[:1], 1)

    each(end, middle)
    group(2)

    def middle(who):
        pass_w(who, 0, parts[:2], 0)
        pass_w(who, 2, parts[1:2], 1)

    each(lambda who: None, middle)
    group(3)

    cross = place(z, 1 - x, y, x)
    own_rows = c == x
    cross_part = (c + x) % 2
    first_part = 2 * (1 - cross_part)

    def att_cross():
        return remote(att.at[2], att.at[cross_part], att_send.at[0], att_recv.at[cross_part], cross)

    def att_near():
        return remote(att.at[2], att.at[1], att_send.at[1], att_recv.at[1], partner)

    att_cross().start()

    @pl.when(jnp.logical_not(own_rows))
    def _():
        att_near().start()

    def att_wait():
        arrive(att.at[1], att_recv.at[1])

        @pl.when(jnp.logical_not(own_rows))
        def _():
            arrive(att.at[0], att_recv.at[0])

    def end(who):
        pass_w(who, 1, parts[:2], None)

    def middle(who):
        pass_w(who, 0, parts[2:], 0)
        pass_w(who, 2, parts[2:], 1)
        for cut, low in parts[2:]:
            w_send_to(who, 1, 1, cut, low)

    each(end, middle)
    att_wait()

    def far_copy(part):
        src = first_part if part == 0 else 1
        return remote(att.at[src], far.at[part], far_send.at[part], far_recv.at[part], inward)

    def end(who):
        for part in range(2):
            go(who, functools.partial(far_copy, part))

    each(end, lambda who: None)

    def sum_copy(k, slot, cut, zz):
        return remote(
            stage.at[slot, cut], sums.at[y, x, cut], sum_send.at[slot, cut], sum_recv.at[y, x, cut],
            {"seq": 2 * zz + c, "head": slab(k)},
        )

    def here(k):
        return own_rows & (slab(k) == head)

    def product(k, cut, first, second):
        added = jnp.dot(first, wbuf[k, cut, :depth, :], preferred_element_type=jnp.float32)
        return added + jnp.dot(second, wbuf[k, cut, depth:, :], preferred_element_type=jnp.float32)

    def project(k, slot, cut):
        value = product(k, cut, att[first_part], att[1]).astype(jnp.bfloat16)

        @pl.when(here(k))
        def _():
            sums[y, x, cut] = value

        @pl.when(jnp.logical_not(here(k)))
        def _():
            stage[slot, cut] = value
            sum_copy(k, slot, cut, z).start()

    def project_far(who, cut):
        stage[slabs, cut] = product(far_slab, cut, far[0], far[1]).astype(jnp.bfloat16)
        go(who, lambda: sum_copy(far_slab, slabs, cut, slab(0)))

    def near_w(k, cut):
        for low in range(2):
            w_wait(1, k, cut, low)

    for cut in cuts:
        near_w(order[0], cut)
        project(order[0], 0, cut)

    near_w(order[1], 0)
    project(order[1], 1, 0)

    def middle(who):
        near_w(0, 1)
        project(0, 1, 1)

    each(lambda who: None, middle)
    for cut in cuts:

        def end(who):
            pass_w(who, 2, [(cut, low) for low in range(2)], None)

        each(end, lambda who: None)
        near_w(2, cut)
        project(2, 2, cut)

    def end(who):
        pass_w(who, 1, parts[2:], None)
        near_w(1, 1)
        project(1, 1, 1)

    def middle(who):
        pass_w(who, 3, parts[:2], None)
        near_w(3, 0)
        project(3, 3, 0)
        pass_w(who, 3, parts[2:], None)
        for part in range(2):
            arrive(far.at[part], far_recv.at[part])
        project_far(who, 0)
        near_w(3, 1)
        project_far(who, 1)
        project(3, 3, 1)

    each(end, middle)

    stays = own_rows & ((role == 1) | (slab(far_slab) != head))
    for cut in cuts:
        for lane in range(2):
            for row in range(2):

                @pl.when(jnp.logical_not(stays & (row == y) & (lane == x)))
                def _():
                    arrive(sums.at[row, lane, cut], sum_recv.at[row, lane, cut])

            at = lane * width + cut * half
            out_ref[:, at : at + half] = (
                sums[0, lane, cut].astype(jnp.float32) + sums[1, lane, cut].astype(jnp.float32)
            ).astype(jnp.bfloat16)

    def finish(who):
        for make in sent[who]:
            make().wait_send()

    each(finish, finish)
    att_cross().wait_send()

    @pl.when(jnp.logical_not(own_rows))
    def _():
        att_near().wait_send()

    for step in range(slabs):
        k = order[step]
        made = jnp.logical_not(here(k))
        if step == far_slab:
            made = made & (role == 1)

        @pl.when(made)
        def _(k=k, step=step):
            for cut in cuts:
                sum_copy(k, step, cut, z).wait_send()


def line_form(n, queries, keys, values, doc_ids, span_order, out_weight):
    rows = queries.shape[0]
    depth, width = out_weight.shape
    half = width // 2
    slabs = n // 2
    heads = queries.shape[1] // DH
    bf16 = jnp.bfloat16
    dma = pltpu.SemaphoreType.DMA
    return pl.pallas_call(
        functools.partial(line_kernel, n),
        out_shape=jax.ShapeDtypeStruct((rows, 2 * width), bf16),
        in_specs=[pl.BlockSpec(memory_space=pl.ANY)] * 6,
        out_specs=pl.BlockSpec(memory_space=pltpu.VMEM),
        scratch_shapes=[
            pltpu.VMEM(queries.shape, bf16),
            pltpu.VMEM((doc_ids.shape[0] // (rows // 2), rows // 2), jnp.int32),
            pltpu.SMEM(span_order.shape, jnp.int32),
            dma((9,)),
            pltpu.VMEM((slabs, 2, rows, DH), bf16),
            pltpu.VMEM((slabs, 2, rows, DH), bf16),
            pltpu.VMEM((slabs, 2, 2 * depth, half), bf16),
            pltpu.VMEM((2, rows, 2 * rows), jnp.float32),
            pltpu.VMEM((heads, rows, DH), jnp.float32),
            pltpu.VMEM((heads, rows, 2 * DH), jnp.float32),
            pltpu.VMEM((3,) + queries.shape, bf16),
            pltpu.VMEM((2,) + queries.shape, bf16),
            pltpu.VMEM((slabs + 1, 2, rows, half), bf16),
            pltpu.VMEM((2, 2, 2, rows, half), bf16),
            dma((2, 3, slabs)),
            dma((2, 2, slabs)),
            dma((3, slabs, 2, 2)),
            dma((2, slabs, 2, 2)),
            dma((2,)),
            dma((2,)),
            dma((2,)),
            dma((2,)),
            dma((slabs + 1, 2)),
            dma((2, 2, 2)),
        ],
        compiler_params=pltpu.CompilerParams(
            collective_id=0, has_side_effects=True, vmem_limit_bytes=62 * 1024 * 1024
        ),
    )(queries, keys, values, doc_ids.reshape(-1, rows // 2), span_order, out_weight)


def on_device(mesh_shape, queries, keys, values, doc_ids, span_order, out_weight):
    n, groups = mesh_shape["seq"], mesh_shape["head"]
    rows = queries.shape[0]
    depth, width = out_weight.shape
    fits = (
        groups == 4
        and n == 2 * groups
        and rows == 2 * DH
        and keys.shape[1] == DH
        and queries.shape[1] == depth
        and depth % (2 * DH) == 0
        and width % (4 * DH) == 0
        and depth * width <= 512 * 512
    )
    if fits:
        return line_form(n, queries, keys, values, doc_ids, span_order, out_weight)
    return gathered_form(queries, keys, values, doc_ids, span_order, out_weight)


def solution(mesh):
    return jax.shard_map(
        functools.partial(on_device, dict(mesh.shape)),
        mesh=mesh,
        in_specs=(P("seq", "head"), P("seq", "head"), P("seq", "head"), P(), P(), P("head", "seq")),
        out_specs=P("seq", "head"),
        check_vma=False,
    )
```

```python
import functools
import math

import jax
import jax.numpy as jnp
from jax import lax
from jax.experimental import pallas as pl
from jax.experimental.pallas import tpu as pltpu
from jax.sharding import PartitionSpec as P

MESH = pl.DeviceIdType.MESH

DH = 128
NEG = -1e30

def gathered_form(queries, keys, values, doc_ids, span_order, out_weight):
    tok_rows = queries.shape[0]
    span = tok_rows // 2
    local_heads = queries.shape[1] // DH
    local_kv = keys.shape[1] // DH
    group_size = local_heads // local_kv
    n_blocks = span_order.shape[0]
    scale = 1.0 / math.sqrt(DH)
    mine = lax.axis_index("seq")
    own_blocks = lax.dynamic_slice_in_dim(span_order, 2 * mine, 2, 0)
    local_rows = jnp.arange(tok_rows, dtype=jnp.int32)
    qpos = jnp.where(local_rows < span, own_blocks[0], own_blocks[1]) * span + local_rows % span
    qdoc = jnp.take(doc_ids, qpos)
    q_heads = queries.reshape(tok_rows, local_kv, group_size, DH)

    def update(state, kblk, vblk, kpos, kdoc):
        largest, total, summed = state
        count = kblk.shape[0]
        k_heads = kblk.reshape(count, local_kv, DH)
        v_heads = vblk.reshape(count, local_kv, DH)
        scores = (
            jnp.einsum("qhgd,khd->hgqk", q_heads, k_heads, preferred_element_type=jnp.float32)
            * scale
        )
        visible = (qdoc[:, None] == kdoc[None, :]) & (kpos[None, :] <= qpos[:, None])
        masked = jnp.where(visible, scores, jnp.float32(-1e30))
        new_largest = jnp.maximum(largest, jnp.max(masked, axis=-1))
        factor = jnp.exp(largest - new_largest)
        weights = jnp.where(visible, jnp.exp(masked - new_largest[..., None]), jnp.float32(0.0))
        total = total * factor + jnp.sum(weights, axis=-1)
        weights_b = weights.astype(jnp.bfloat16)
        added = jnp.einsum("hgqk,khd->qhgd", weights_b, v_heads, preferred_element_type=jnp.float32)
        summed = summed * jnp.transpose(factor, (2, 0, 1))[..., None] + added
        return (new_largest, total, summed)

    initial = (
        jnp.full((local_kv, group_size, tok_rows), -1e30, jnp.float32),
        jnp.zeros((local_kv, group_size, tok_rows), jnp.float32),
        jnp.zeros((tok_rows, local_kv, group_size, DH), jnp.float32),
    )
    state = initial
    kpiece = lax.all_gather(keys, "seq", axis=0, tiled=True)
    vpiece = lax.all_gather(values, "seq", axis=0, tiled=True)
    count = kpiece.shape[0]
    width = math.gcd(count, 1024)
    steps = count // width
    rows = jnp.arange(count, dtype=jnp.int32)
    match = (rows // span)[:, None] == jnp.arange(n_blocks, dtype=jnp.int32)[None, :]
    owner = jnp.sum(jnp.where(match, span_order[None, :], 0), axis=1)
    kpos = owner * span + rows % span
    kdoc = jnp.take(doc_ids, kpos)
    kparts = kpiece.reshape(steps, width, kpiece.shape[1])
    vparts = vpiece.reshape(steps, width, vpiece.shape[1])

    def one_step(carry, items):
        kblk, vblk, pblk, dblk = items
        carry = update(carry, kblk, vblk, pblk, dblk)
        return (carry, None)

    state, unused = lax.scan(
        one_step, state, (kparts, vparts, kpos.reshape(steps, width), kdoc.reshape(steps, width))
    )
    largest, total, summed = state
    attended = (summed / jnp.transpose(total, (2, 0, 1))[..., None]).astype(jnp.bfloat16)
    attended = attended.reshape(tok_rows, local_heads * DH)
    partial_out = jnp.dot(
        attended,
        lax.all_gather(out_weight, "seq", axis=1, tiled=True),
        preferred_element_type=jnp.float32,
    )
    return lax.psum_scatter(
        partial_out.astype(jnp.bfloat16), "head", scatter_dimension=1, tiled=True
    )


def line_kernel(
    n, q_in, k_in, v_in, doc_in, order_in, w_in, out_ref,
    q_ref, doc_ref, order_ref, fetched, kbuf, vbuf, wbuf, bias, best, acc, att, far, stage,
    kv_send, kv_recv, w_send, w_recv, att_send, att_recv, far_send, far_recv, sum_send, sum_recv,
):
    seq, head = lax.axis_index("seq"), lax.axis_index("head")
    z, x, y, c = seq // 2, seq % 2, head // 2, head % 2
    side = z // 2
    role = (z + side) % 2
    rows = q_ref.shape[0]
    span = rows // 2
    heads = q_ref.shape[1] // DH
    depth, width = w_in.shape
    half, deep = width // 2, depth // 2
    factor = math.log2(math.e) / math.sqrt(DH)
    slabs = n // 2
    far_slab = slabs - 1
    cuts = range(2)
    parts = [(cut, low) for cut in range(2) for low in range(2)]

    def slab(k):
        return k + side * (slabs - 1 - 2 * k)

    def place(zz, xx, yy, cc):
        return {"seq": 2 * zz + xx, "head": 2 * yy + cc}

    inward = place((1 - role) * slab(1) + role * slab(2), x, y, c)
    outward = place(slab(0), x, y, c)
    across = {"seq": 2 * z + 1 - x}
    partner = {"head": 2 * y + 1 - c}
    ways = (inward, outward, across)

    own = role
    fetches = [
        pltpu.make_async_copy(src, dst, fetched.at[at])
        for at, (src, dst) in enumerate(
            [(k_in, kbuf.at[own, 0]), (v_in, vbuf.at[own, 0])]
            + [
                (w_in.at[pl.ds(low * deep, deep), pl.ds(cut * half, half)], wbuf.at[own, cut, pl.ds(low * deep, deep)])
                for cut, low in parts
            ]
            + [(doc_in, doc_ref), (order_in, order_ref), (q_in, q_ref)]
        )
    ]
    for fetch in fetches:
        fetch.start()

    barrier = pltpu.get_barrier_semaphore()
    for zz in range(2):
        for flip in range(8):
            fx, fy, fc = flip // 4, flip // 2 % 2, flip % 2
            if zz or flip:
                there = place((z - 2 * side + zz) % 2 + 2 * side, (x + fx) % 2, (y + fy) % 2, (c + fc) % 2)
                pl.semaphore_signal(barrier, inc=1, device_id=there, device_id_type=MESH)

    @pl.when(role == 1)
    def _():
        pl.semaphore_signal(barrier, inc=1, device_id=inward, device_id_type=MESH)

    pl.semaphore_wait(barrier, 15 + role)

    def remote(src, dst, send, recv, device):
        return pltpu.make_async_remote_copy(
            src_ref=src, dst_ref=dst, send_sem=send, recv_sem=recv, device_id=device, device_id_type=MESH
        )

    sent = ([], [])

    def go(who, make):
        make().start()
        sent[who].append(make)

    def arrive(dst, recv):
        remote(dst, dst, att_send.at[0], recv, partner).wait_recv()

    def kv_send_to(who, which, way, k):
        buf = (kbuf, vbuf)[which]
        to = slabs - 1 - k if (who == 1 and way == 0) else k
        lane = 1 if way == 2 else 0
        go(
            who,
            lambda: remote(
                buf.at[k, 0], buf.at[to, lane], kv_send.at[which, way, k], kv_recv.at[which, lane, to], ways[way]
            ),
        )

    def kv_wait(which, lane, k):
        arrive((kbuf, vbuf)[which].at[k, lane], kv_recv.at[which, lane, k])

    def w_at(k, cut, low, mine):
        return wbuf.at[k, cut, pl.ds(mine * depth + low * deep, deep)]

    def w_send_to(who, way, k, cut, low):
        to = slabs - 1 - k if (who == 1 and way == 0) else k
        mine = 1 if way == 2 else 0
        go(
            who,
            lambda: remote(
                w_at(k, cut, low, 0), w_at(to, cut, low, mine), w_send.at[way, k, cut, low],
                w_recv.at[mine, to, cut, low], partner if way == 2 else ways[way],
            ),
        )

    def w_wait(mine, k, cut, low):
        arrive(w_at(k, cut, low, mine), w_recv.at[mine, k, cut, low])

    def each(end, middle):
        @pl.when(role == 0)
        def _():
            end(0)

        @pl.when(role == 1)
        def _():
            middle(1)

    for which in range(2):
        fetches[which].wait()

        def end(who):
            for way in (0, 2):
                kv_send_to(who, which, way, 0)

        def middle(who):
            for way in (1, 0, 2):
                kv_send_to(who, which, way, 1)

        each(end, middle)
    for fetch in fetches[2:]:
        fetch.wait()

    def middle(who):
        w_send_to(who, 1, 1, *parts[0])

    each(lambda who: None, middle)


    down = lax.broadcasted_iota(jnp.int32, (span, span), 0)
    along = lax.broadcasted_iota(jnp.int32, (span, span), 1)
    query_at, query_doc = [], []
    for part in range(2):
        block = order_ref[2 * seq + part]
        query_at.append(down + block * span)
        docs = doc_ref[pl.ds(block, 1), :].astype(jnp.float32)
        query_doc.append(jnp.transpose(jnp.broadcast_to(docs, (span, span))))

    order = (role, 1 - role, 2, 3)

    def mask(step):
        for lane in range(2):
            source = 2 * slab(order[step]) + (x if lane == 0 else 1 - x)
            for j in range(2):
                block = order_ref[2 * source + j]
                docs = doc_ref[pl.ds(block, 1), :].astype(jnp.float32)
                key_at = along + block * span
                first = (2 * lane + j) * span
                for part in range(2):
                    seen = (query_doc[part] == docs) & (key_at <= query_at[part])
                    bias[step % 2, part * span : (part + 1) * span, first : first + span] = jnp.where(
                        seen, jnp.float32(0.0), jnp.float32(NEG)
                    )

    def attend(step, h):
        k = order[step]
        count = 2 * rows
        q = q_ref[:, h * DH : (h + 1) * DH]
        scores = lax.dot_general(
            q, kbuf[k].reshape(count, DH), (((1,), (1,)), ((), ())), preferred_element_type=jnp.float32
        )
        masked = scores * factor + bias[step % 2]
        top = jnp.broadcast_to(jnp.max(masked, axis=-1, keepdims=True), (rows, DH))
        if step > 0:
            before = best[h]
            top = jnp.maximum(before, top)
        weights = jnp.concatenate(
            [jnp.exp2(masked[:, at : at + DH] - top).astype(jnp.bfloat16) for at in range(0, count, DH)], axis=1
        )
        wide = jnp.concatenate([vbuf[k].reshape(count, DH), jnp.ones((count, DH), jnp.bfloat16)], axis=1)
        summed = jnp.dot(weights, wide, preferred_element_type=jnp.float32)
        if step > 0:
            fade = jnp.exp2(before - top)
            summed = summed + acc[h] * jnp.concatenate([fade, fade], axis=1)
        if step < slabs - 1:
            best[h] = top
            acc[h] = summed
        else:
            att[2, :, h * DH : (h + 1) * DH] = (summed[:, :DH] / summed[:, DH:]).astype(jnp.bfloat16)

    def group(step):
        for which in range(2):
            kv_wait(which, 1, order[step])
        for h in range(heads):
            attend(step, h)

    mask(0)

    def end(who):
        for which in range(2):
            kv_wait(which, 0, 1)
            kv_send_to(who, which, 2, 1)
        for cut, low in parts:
            w_send_to(who, 0, 0, cut, low)
        for cut, low in parts:
            w_send_to(who, 2, 0, cut, low)

    def middle(who):
        for which in range(2):
            kv_wait(which, 0, 0)
            kv_send_to(who, which, 0, 0)
            kv_send_to(who, which, 2, 0)
            kv_wait(which, 0, 2)
            kv_send_to(who, which, 1, 2)
            kv_send_to(who, which, 2, 2)
        for cut, low in parts:
            w_send_to(who, 0, 1, cut, low)
        for which in range(2):
            kv_wait(which, 0, 3)
            kv_send_to(who, which, 1, 3)
            kv_send_to(who, which, 2, 3)
        w_send_to(who, 1, 1, *parts[1])
        for cut, low in parts:
            w_send_to(who, 2, 1, cut, low)

    each(end, middle)
    mask(1)
    group(0)

    def end(who):
        for which in range(2):
            kv_wait(which, 0, 2)
            kv_send_to(who, which, 2, 2)

    each(end, lambda who: None)
    group(1)
    mask(2)
    mask(3)

    def pass_w(who, k, which, way):
        for cut, low in which:
            w_wait(0, k, cut, low)
            if way is not None:
                w_send_to(who, way, k, cut, low)
            w_send_to(who, 2, k, cut, low)

    def end(who):
        for which in range(2):
            kv_wait(which, 0, 3)
            kv_send_to(who, which, 2, 3)

    def middle(who):
        pass_w(who, 2, parts[:1], 1)

    each(end, middle)
    group(2)

    def middle(who):
        pass_w(who, 0, parts[:2], 0)
        pass_w(who, 2, parts[1:2], 1)

    each(lambda who: None, middle)
    group(3)

    cross = place(z, 1 - x, y, x)
    own_rows = c == x
    cross_part = (c + x) % 2
    first_part = 2 * (1 - cross_part)

    def att_cross():
        return remote(att.at[2], att.at[cross_part], att_send.at[0], att_recv.at[cross_part], cross)

    def att_near():
        return remote(att.at[2], att.at[1], att_send.at[1], att_recv.at[1], partner)

    att_cross().start()

    @pl.when(jnp.logical_not(own_rows))
    def _():
        att_near().start()

    def far_copy(part):
        return remote(att.at[part], far.at[part], far_send.at[part], far_recv.at[part], inward)

    def own_far():
        return remote(att.at[2], far.at[0], far_send.at[0], far_recv.at[0], inward)

    @pl.when(own_rows & (role == 0))
    def _():
        own_far().start()

    def end(who):
        pass_w(who, 1, parts[:2], None)

    def middle(who):
        pass_w(who, 0, parts[2:], 0)
        pass_w(who, 2, parts[2:], 1)
        for cut, low in parts[2:]:
            w_send_to(who, 1, 1, cut, low)

    each(end, middle)

    for part in (1 - c, c):

        @pl.when(own_rows & (part == 1))
        def _():
            arrive(att.at[1], att_recv.at[1])

        @pl.when(jnp.logical_not(own_rows))
        def _(part=part):
            arrive(att.at[part], att_recv.at[part])

        @pl.when((role == 0) & (jnp.logical_not(own_rows) | (part == 1)))
        def _(part=part):
            far_copy(part).start()

    def sum_at(row, lane, cut):
        return out_ref.at[row, :, pl.ds(pl.multiple_of(lane * width + cut * half, half), half)]

    def sum_copy(k, slot, cut, zz):
        return remote(
            stage.at[slot, cut], sum_at(y, x, cut), sum_send.at[slot, cut], sum_recv.at[y, x, cut],
            {"seq": 2 * zz + c, "head": slab(k)},
        )

    def sum_stay(slot, cut):
        return pltpu.make_async_copy(stage.at[slot, cut], sum_at(y, x, cut), sum_send.at[slot, cut])

    def here(k):
        return own_rows & (slab(k) == head)

    def product(k, cut, first, second):
        added = jnp.dot(first, wbuf[k, cut, :depth, :], preferred_element_type=jnp.float32)
        return added + jnp.dot(second, wbuf[k, cut, depth:, :], preferred_element_type=jnp.float32)

    def project(k, slot, cut):
        value = product(k, cut, att[first_part], att[1]).astype(jnp.bfloat16)

        stage[slot, cut] = value

        @pl.when(here(k))
        def _():
            sum_stay(slot, cut).start()

        @pl.when(jnp.logical_not(here(k)))
        def _():
            sum_copy(k, slot, cut, z).start()

    def project_far(who, cut):
        stage[slabs, cut] = product(far_slab, cut, far[0], far[1]).astype(jnp.bfloat16)
        go(who, lambda: sum_copy(far_slab, slabs, cut, slab(0)))

    def near_w(k, cut):
        for low in range(2):
            w_wait(1, k, cut, low)

    for cut in cuts:
        near_w(order[0], cut)
        project(order[0], 0, cut)

    near_w(order[1], 0)
    project(order[1], 1, 0)

    def middle(who):
        near_w(0, 1)
        project(0, 1, 1)

    each(lambda who: None, middle)
    for cut in cuts:

        def end(who):
            pass_w(who, 2, [(cut, low) for low in range(2)], None)

        each(end, lambda who: None)
        near_w(2, cut)
        project(2, 2, cut)

    def end(who):
        pass_w(who, 1, parts[2:], None)
        near_w(1, 1)
        project(1, 1, 1)

    def middle(who):
        pass_w(who, 3, parts[:2], None)
        near_w(3, 0)
        project(3, 3, 0)
        pass_w(who, 3, parts[2:], None)
        for part in range(2):
            arrive(far.at[part], far_recv.at[part])
        project_far(who, 0)
        near_w(3, 1)
        project_far(who, 1)
        project(3, 3, 1)

    each(end, middle)

    stays = own_rows & ((role == 1) | (slab(far_slab) != head))
    for cut in cuts:
        for lane in range(2):
            for row in range(2):

                @pl.when(jnp.logical_not(stays & (row == y) & (lane == x)))
                def _():
                    arrive(sum_at(row, lane, cut), sum_recv.at[row, lane, cut])

    def finish(who):
        for make in sent[who]:
            make().wait_send()

    each(finish, finish)

    @pl.when(role == 0)
    def _():
        for part in range(2):
            far_copy(part).wait_send()

    att_cross().wait_send()

    @pl.when(jnp.logical_not(own_rows))
    def _():
        att_near().wait_send()

    for step in range(slabs):
        k = order[step]
        made = (role == 1) | (step != far_slab)

        @pl.when(made & jnp.logical_not(here(k)))
        def _(k=k, step=step):
            for cut in cuts:
                sum_copy(k, step, cut, z).wait_send()

        @pl.when(made & here(k))
        def _(step=step):
            for cut in cuts:
                sum_stay(step, cut).wait()


def line_form(n, queries, keys, values, doc_ids, span_order, out_weight):
    rows = queries.shape[0]
    depth, width = out_weight.shape
    half = width // 2
    slabs = n // 2
    heads = queries.shape[1] // DH
    bf16 = jnp.bfloat16
    dma = pltpu.SemaphoreType.DMA
    sums = pl.pallas_call(
        functools.partial(line_kernel, n),
        out_shape=jax.ShapeDtypeStruct((2, rows, 2 * width), bf16),
        in_specs=[pl.BlockSpec(memory_space=pl.ANY)] * 6,
        out_specs=pl.BlockSpec(memory_space=pl.ANY),
        scratch_shapes=[
            pltpu.VMEM(queries.shape, bf16),
            pltpu.VMEM((doc_ids.shape[0] // (rows // 2), rows // 2), jnp.int32),
            pltpu.SMEM(span_order.shape, jnp.int32),
            dma((9,)),
            pltpu.VMEM((slabs, 2, rows, DH), bf16),
            pltpu.VMEM((slabs, 2, rows, DH), bf16),
            pltpu.VMEM((slabs, 2, 2 * depth, half), bf16),
            pltpu.VMEM((2, rows, 2 * rows), jnp.float32),
            pltpu.VMEM((heads, rows, DH), jnp.float32),
            pltpu.VMEM((heads, rows, 2 * DH), jnp.float32),
            pltpu.VMEM((3,) + queries.shape, bf16),
            pltpu.VMEM((2,) + queries.shape, bf16),
            pltpu.VMEM((slabs + 1, 2, rows, half), bf16),
            dma((2, 3, slabs)),
            dma((2, 2, slabs)),
            dma((3, slabs, 2, 2)),
            dma((2, slabs, 2, 2)),
            dma((2,)),
            dma((2,)),
            dma((2,)),
            dma((2,)),
            dma((slabs + 1, 2)),
            dma((2, 2, 2)),
        ],
        compiler_params=pltpu.CompilerParams(
            collective_id=0, has_side_effects=True, vmem_limit_bytes=62 * 1024 * 1024
        ),
    )(queries, keys, values, doc_ids.reshape(-1, rows // 2), span_order, out_weight)
    return (sums[0].astype(jnp.float32) + sums[1].astype(jnp.float32)).astype(bf16)


def on_device(mesh_shape, queries, keys, values, doc_ids, span_order, out_weight):
    n, groups = mesh_shape["seq"], mesh_shape["head"]
    rows = queries.shape[0]
    depth, width = out_weight.shape
    fits = (
        groups == 4
        and n == 2 * groups
        and rows == 2 * DH
        and keys.shape[1] == DH
        and queries.shape[1] == depth
        and depth % (2 * DH) == 0
        and width % (4 * DH) == 0
        and depth * width <= 512 * 512
    )
    if fits:
        return line_form(n, queries, keys, values, doc_ids, span_order, out_weight)
    return gathered_form(queries, keys, values, doc_ids, span_order, out_weight)


def solution(mesh):
    return jax.shard_map(
        functools.partial(on_device, dict(mesh.shape)),
        mesh=mesh,
        in_specs=(P("seq", "head"), P("seq", "head"), P("seq", "head"), P(), P(), P("head", "seq")),
        out_specs=P("seq", "head"),
        check_vma=False,
    )
```

```python
import functools
import math

import jax
import jax.numpy as jnp
from jax import lax
from jax.experimental import pallas as pl
from jax.experimental.pallas import tpu as pltpu
from jax.sharding import PartitionSpec as P

MESH = pl.DeviceIdType.MESH

DH = 128
NEG = -1e30

def gathered_form(queries, keys, values, doc_ids, span_order, out_weight):
    tok_rows = queries.shape[0]
    span = tok_rows // 2
    local_heads = queries.shape[1] // DH
    local_kv = keys.shape[1] // DH
    group_size = local_heads // local_kv
    n_blocks = span_order.shape[0]
    scale = 1.0 / math.sqrt(DH)
    mine = lax.axis_index("seq")
    own_blocks = lax.dynamic_slice_in_dim(span_order, 2 * mine, 2, 0)
    local_rows = jnp.arange(tok_rows, dtype=jnp.int32)
    qpos = jnp.where(local_rows < span, own_blocks[0], own_blocks[1]) * span + local_rows % span
    qdoc = jnp.take(doc_ids, qpos)
    q_heads = queries.reshape(tok_rows, local_kv, group_size, DH)

    def update(state, kblk, vblk, kpos, kdoc):
        largest, total, summed = state
        count = kblk.shape[0]
        k_heads = kblk.reshape(count, local_kv, DH)
        v_heads = vblk.reshape(count, local_kv, DH)
        scores = (
            jnp.einsum("qhgd,khd->hgqk", q_heads, k_heads, preferred_element_type=jnp.float32)
            * scale
        )
        visible = (qdoc[:, None] == kdoc[None, :]) & (kpos[None, :] <= qpos[:, None])
        masked = jnp.where(visible, scores, jnp.float32(-1e30))
        new_largest = jnp.maximum(largest, jnp.max(masked, axis=-1))
        factor = jnp.exp(largest - new_largest)
        weights = jnp.where(visible, jnp.exp(masked - new_largest[..., None]), jnp.float32(0.0))
        total = total * factor + jnp.sum(weights, axis=-1)
        weights_b = weights.astype(jnp.bfloat16)
        added = jnp.einsum("hgqk,khd->qhgd", weights_b, v_heads, preferred_element_type=jnp.float32)
        summed = summed * jnp.transpose(factor, (2, 0, 1))[..., None] + added
        return (new_largest, total, summed)

    initial = (
        jnp.full((local_kv, group_size, tok_rows), -1e30, jnp.float32),
        jnp.zeros((local_kv, group_size, tok_rows), jnp.float32),
        jnp.zeros((tok_rows, local_kv, group_size, DH), jnp.float32),
    )
    state = initial
    kpiece = lax.all_gather(keys, "seq", axis=0, tiled=True)
    vpiece = lax.all_gather(values, "seq", axis=0, tiled=True)
    count = kpiece.shape[0]
    width = math.gcd(count, 1024)
    steps = count // width
    rows = jnp.arange(count, dtype=jnp.int32)
    match = (rows // span)[:, None] == jnp.arange(n_blocks, dtype=jnp.int32)[None, :]
    owner = jnp.sum(jnp.where(match, span_order[None, :], 0), axis=1)
    kpos = owner * span + rows % span
    kdoc = jnp.take(doc_ids, kpos)
    kparts = kpiece.reshape(steps, width, kpiece.shape[1])
    vparts = vpiece.reshape(steps, width, vpiece.shape[1])

    def one_step(carry, items):
        kblk, vblk, pblk, dblk = items
        carry = update(carry, kblk, vblk, pblk, dblk)
        return (carry, None)

    state, unused = lax.scan(
        one_step, state, (kparts, vparts, kpos.reshape(steps, width), kdoc.reshape(steps, width))
    )
    largest, total, summed = state
    attended = (summed / jnp.transpose(total, (2, 0, 1))[..., None]).astype(jnp.bfloat16)
    attended = attended.reshape(tok_rows, local_heads * DH)
    partial_out = jnp.dot(
        attended,
        lax.all_gather(out_weight, "seq", axis=1, tiled=True),
        preferred_element_type=jnp.float32,
    )
    return lax.psum_scatter(
        partial_out.astype(jnp.bfloat16), "head", scatter_dimension=1, tiled=True
    )


def line_kernel(
    n, q_in, k_in, v_in, doc_in, order_in, w_in, out_ref,
    q_ref, doc_ref, order_ref, fetched, kbuf, vbuf, wbuf, bias, best, acc, att, far, stage,
    kv_send, kv_recv, w_send, w_recv, att_send, att_recv, far_send, far_recv, sum_send, sum_recv,
):
    seq, head = lax.axis_index("seq"), lax.axis_index("head")
    z, x, y, c = seq // 2, seq % 2, head // 2, head % 2
    side = z // 2
    role = (z + side) % 2
    rows = q_ref.shape[0]
    span = rows // 2
    heads = q_ref.shape[1] // DH
    depth, width = w_in.shape
    half, deep = width // 2, depth // 2
    factor = math.log2(math.e) / math.sqrt(DH)
    slabs = n // 2
    far_slab = slabs - 1
    cuts = range(2)
    parts = [(cut, low) for cut in range(2) for low in range(2)]

    def slab(k):
        return k + side * (slabs - 1 - 2 * k)

    def place(zz, xx, yy, cc):
        return {"seq": 2 * zz + xx, "head": 2 * yy + cc}

    inward = place((1 - role) * slab(1) + role * slab(2), x, y, c)
    outward = place(slab(0), x, y, c)
    across = {"seq": 2 * z + 1 - x}
    partner = {"head": 2 * y + 1 - c}
    ways = (inward, outward, across)

    own = role
    fetches = [
        pltpu.make_async_copy(src, dst, fetched.at[at])
        for at, (src, dst) in enumerate(
            [(k_in, kbuf.at[own, 0]), (v_in, vbuf.at[own, 0])]
            + [(w_in.at[:, pl.ds(cut * half, half)], wbuf.at[own, cut, pl.ds(0, depth)]) for cut in range(2)]
            + [(doc_in, doc_ref), (order_in, order_ref), (q_in, q_ref)]
        )
    ]
    for fetch in fetches:
        fetch.start()

    barrier = pltpu.get_barrier_semaphore()
    for zz in range(2):
        for flip in range(8):
            fx, fy, fc = flip // 4, flip // 2 % 2, flip % 2
            if zz or flip:
                there = place((z - 2 * side + zz) % 2 + 2 * side, (x + fx) % 2, (y + fy) % 2, (c + fc) % 2)
                pl.semaphore_signal(barrier, inc=1, device_id=there, device_id_type=MESH)

    @pl.when(role == 1)
    def _():
        pl.semaphore_signal(barrier, inc=1, device_id=inward, device_id_type=MESH)

    pl.semaphore_wait(barrier, 15 + role)

    def remote(src, dst, send, recv, device):
        return pltpu.make_async_remote_copy(
            src_ref=src, dst_ref=dst, send_sem=send, recv_sem=recv, device_id=device, device_id_type=MESH
        )

    passed, pieces = [0, 0], [0, 0]

    def arrive(dst, recv):
        remote(dst, dst, att_send.at[0], recv, partner).wait_recv()

    def kv_send_to(who, which, way, k):
        buf = (kbuf, vbuf)[which]
        to = slabs - 1 - k if (who == 1 and way == 0) else k
        lane = 1 if way == 2 else 0
        at = which if lane == 0 else 2
        remote(buf.at[k, 0], buf.at[to, lane], kv_send, kv_recv.at[at, to], ways[way]).start()
        passed[who] += 1

    def kv_wait(which, k):
        arrive((kbuf, vbuf)[which].at[k, 0], kv_recv.at[which, k])

    def kv_pair_wait(k):
        both = q_ref.at[:, pl.ds(0, 2 * DH)]
        arrive(both, kv_recv.at[2, k])

    def w_at(k, cut, low, mine):
        return wbuf.at[k, cut, pl.ds(mine * depth + low * deep, deep)]

    def w_send_to(who, way, k, cut, low):
        to = slabs - 1 - k if (who == 1 and way == 0) else k
        mine = 1 if way == 2 else 0
        remote(
            w_at(k, cut, low, 0), w_at(to, cut, low, mine), w_send, w_recv.at[mine, to, cut, 0 if mine else low],
            partner if way == 2 else ways[way],
        ).start()
        pieces[who] += 1

    def w_wait(k, cut, low):
        arrive(w_at(k, cut, low, 0), w_recv.at[0, k, cut, low])

    def each(end, middle):
        @pl.when(role == 0)
        def _():
            end(0)

        @pl.when(role == 1)
        def _():
            middle(1)

    for which in range(2):
        fetches[which].wait()

        def end(who):
            for way in (0, 2):
                kv_send_to(who, which, way, 0)

        def middle(who):
            for way in (1, 0, 2):
                kv_send_to(who, which, way, 1)

        each(end, middle)
    for fetch in fetches[2:]:
        fetch.wait()

    def middle(who):
        w_send_to(who, 1, 1, *parts[0])

    each(lambda who: None, middle)


    down = lax.broadcasted_iota(jnp.int32, (span, span), 0)
    along = lax.broadcasted_iota(jnp.int32, (span, span), 1)
    query_at, query_doc = [], []
    for part in range(2):
        block = order_ref[2 * seq + part]
        query_at.append(down + block * span)
        docs = doc_ref[pl.ds(block, 1), :].astype(jnp.float32)
        query_doc.append(jnp.transpose(jnp.broadcast_to(docs, (span, span))))

    order = (role, 1 - role, 2, 3)

    def mask(step):
        for lane in range(2):
            source = 2 * slab(order[step]) + (x if lane == 0 else 1 - x)
            for j in range(2):
                block = order_ref[2 * source + j]
                docs = doc_ref[pl.ds(block, 1), :].astype(jnp.float32)
                key_at = along + block * span
                first = (2 * lane + j) * span
                for part in range(2):
                    seen = (query_doc[part] == docs) & (key_at <= query_at[part])
                    bias[step % 2, part * span : (part + 1) * span, first : first + span] = jnp.where(
                        seen, jnp.float32(0.0), jnp.float32(NEG)
                    )

    def attend(step, h):
        k = order[step]
        count = 2 * rows
        q = q_ref[:, h * DH : (h + 1) * DH]
        scores = lax.dot_general(
            q, kbuf[k].reshape(count, DH), (((1,), (1,)), ((), ())), preferred_element_type=jnp.float32
        )
        masked = scores * factor + bias[step % 2]
        top = jnp.broadcast_to(jnp.max(masked, axis=-1, keepdims=True), (rows, DH))
        if step > 0:
            before = best[h]
            top = jnp.maximum(before, top)
        weights = jnp.concatenate(
            [jnp.exp2(masked[:, at : at + DH] - top).astype(jnp.bfloat16) for at in range(0, count, DH)], axis=1
        )
        wide = jnp.concatenate([vbuf[k].reshape(count, DH), jnp.ones((count, DH), jnp.bfloat16)], axis=1)
        summed = jnp.dot(weights, wide, preferred_element_type=jnp.float32)
        if step > 0:
            fade = jnp.exp2(before - top)
            summed = summed + acc[h] * jnp.concatenate([fade, fade], axis=1)
        if step < slabs - 1:
            best[h] = top
            acc[h] = summed
        else:
            att[2, :, h * DH : (h + 1) * DH] = (summed[:, :DH] / summed[:, DH:]).astype(jnp.bfloat16)

    def group(step):
        kv_pair_wait(order[step])
        for h in range(heads):
            attend(step, h)

    mask(0)

    def end(who):
        for which in range(2):
            kv_wait(which, 1)
            kv_send_to(who, which, 2, 1)
        for cut, low in parts:
            w_send_to(who, 0, 0, cut, low)
        for cut, low in parts:
            w_send_to(who, 2, 0, cut, low)

    def middle(who):
        for which in range(2):
            kv_wait(which, 0)
            kv_send_to(who, which, 0, 0)
            kv_send_to(who, which, 2, 0)
            kv_wait(which, 2)
            kv_send_to(who, which, 1, 2)
            kv_send_to(who, which, 2, 2)
        for cut, low in parts:
            w_send_to(who, 0, 1, cut, low)
        for which in range(2):
            kv_wait(which, 3)
            kv_send_to(who, which, 1, 3)
            kv_send_to(who, which, 2, 3)
        w_send_to(who, 1, 1, *parts[1])
        for cut, low in parts:
            w_send_to(who, 2, 1, cut, low)

    each(end, middle)
    mask(1)
    group(0)

    def end(who):
        for which in range(2):
            kv_wait(which, 2)
            kv_send_to(who, which, 2, 2)

    each(end, lambda who: None)
    group(1)
    mask(2)
    mask(3)

    def pass_w(who, k, which, way):
        for cut, low in which:
            w_wait(k, cut, low)
            if way is not None:
                w_send_to(who, way, k, cut, low)
            w_send_to(who, 2, k, cut, low)

    def end(who):
        for which in range(2):
            kv_wait(which, 3)
            kv_send_to(who, which, 2, 3)

    def middle(who):
        pass_w(who, 2, parts[:1], 1)

    each(end, middle)
    group(2)

    def middle(who):
        pass_w(who, 0, parts[:2], 0)
        pass_w(who, 2, parts[1:2], 1)

    each(lambda who: None, middle)
    group(3)

    cross = place(z, 1 - x, y, x)
    own_rows = c == x
    cross_part = (c + x) % 2
    first_part = 2 * (1 - cross_part)

    def att_cross():
        return remote(att.at[2], att.at[cross_part], att_send.at[0], att_recv.at[cross_part], cross)

    def att_near():
        return remote(att.at[2], att.at[1], att_send.at[1], att_recv.at[1], partner)

    att_cross().start()

    @pl.when(jnp.logical_not(own_rows))
    def _():
        att_near().start()

    def far_copy(part):
        return remote(att.at[part], far.at[part], far_send, far_recv, inward)

    def own_far():
        return remote(att.at[2], far.at[0], far_send, far_recv, inward)

    @pl.when(own_rows & (role == 0))
    def _():
        own_far().start()

    def end(who):
        pass_w(who, 1, parts[:2], None)

    def middle(who):
        pass_w(who, 0, parts[2:], 0)
        pass_w(who, 2, parts[2:], 1)
        for cut, low in parts[2:]:
            w_send_to(who, 1, 1, cut, low)

    each(end, middle)

    for part in (1 - c, c):

        @pl.when(own_rows & (part == 1))
        def _():
            arrive(att.at[1], att_recv.at[1])

        @pl.when(jnp.logical_not(own_rows))
        def _(part=part):
            arrive(att.at[part], att_recv.at[part])

        @pl.when((role == 0) & (jnp.logical_not(own_rows) | (part == 1)))
        def _(part=part):
            far_copy(part).start()

    def sum_at(row, lane, cut):
        return out_ref.at[row, :, pl.ds(pl.multiple_of(lane * width + cut * half, half), half)]

    def sum_copy(k, slot, cut, zz):
        return remote(
            stage.at[slot, cut], sum_at(y, x, cut), sum_send, sum_recv,
            {"seq": 2 * zz + c, "head": slab(k)},
        )

    def sum_stay(slot, cut):
        return pltpu.make_async_copy(stage.at[slot, cut], sum_at(y, x, cut), sum_recv)

    def here(k):
        return own_rows & (slab(k) == head)

    def product(k, cut, first, second):
        added = jnp.dot(first, wbuf[k, cut, :depth, :], preferred_element_type=jnp.float32)
        return added + jnp.dot(second, wbuf[k, cut, depth:, :], preferred_element_type=jnp.float32)

    def project(k, slot, cut):
        value = product(k, cut, att[first_part], att[1]).astype(jnp.bfloat16)

        stage[slot, cut] = value

        @pl.when(here(k))
        def _():
            sum_stay(slot, cut).start()

        @pl.when(jnp.logical_not(here(k)))
        def _():
            sum_copy(k, slot, cut, z).start()

    def project_far(who, cut):
        stage[slabs, cut] = product(far_slab, cut, far[0], far[1]).astype(jnp.bfloat16)
        sum_copy(far_slab, slabs, cut, slab(0)).start()

    def near_w(k, cut):
        arrive(wbuf.at[k, cut, pl.ds(depth, depth)], w_recv.at[1, k, cut, 0])

    for cut in cuts:
        near_w(order[0], cut)
        project(order[0], 0, cut)

    near_w(order[1], 0)
    project(order[1], 1, 0)

    def middle(who):
        near_w(0, 1)
        project(0, 1, 1)

    each(lambda who: None, middle)
    for cut in cuts:

        def end(who):
            pass_w(who, 2, [(cut, low) for low in range(2)], None)

        each(end, lambda who: None)
        near_w(2, cut)
        project(2, 2, cut)

    def end(who):
        pass_w(who, 1, parts[2:], None)
        near_w(1, 1)
        project(1, 1, 1)

    def middle(who):
        pass_w(who, 3, parts[:2], None)
        near_w(3, 0)
        project(3, 3, 0)
        pass_w(who, 3, parts[2:], None)
        arrive(far, far_recv)
        project_far(who, 0)
        near_w(3, 1)
        project_far(who, 1)
        project(3, 3, 1)

    each(end, middle)

    stays = own_rows & ((role == 1) | (slab(far_slab) != head))

    def left(ref, send):
        remote(ref, ref, send, sum_recv, partner).wait_send()

    def finish(who):
        left(wbuf.at[:2, :, pl.ds(0, passed[who] * rows * DH // (4 * half))], kv_send)
        left(wbuf.at[: pieces[who] // (2 * len(parts))], w_send)
        made = 2 * slabs + 2 if who == 1 else 2 * slabs - 2

        @pl.when(stays)
        def _():
            left(stage.at[: made // 2 - 1], sum_send)

        @pl.when(jnp.logical_not(stays))
        def _():
            left(stage.at[: made // 2], sum_send)

    def end(who):
        left(far, far_send)
        finish(who)

    each(end, finish)
    att_cross().wait_send()

    @pl.when(jnp.logical_not(own_rows))
    def _():
        att_near().wait_send()

    arrive(out_ref, sum_recv)


def line_form(n, queries, keys, values, doc_ids, span_order, out_weight):
    rows = queries.shape[0]
    depth, width = out_weight.shape
    half = width // 2
    slabs = n // 2
    heads = queries.shape[1] // DH
    bf16 = jnp.bfloat16
    dma = pltpu.SemaphoreType.DMA
    sums = pl.pallas_call(
        functools.partial(line_kernel, n),
        out_shape=jax.ShapeDtypeStruct((2, rows, 2 * width), bf16),
        in_specs=[pl.BlockSpec(memory_space=pl.ANY)] * 6,
        out_specs=pl.BlockSpec(memory_space=pl.ANY),
        scratch_shapes=[
            pltpu.VMEM(queries.shape, bf16),
            pltpu.VMEM((doc_ids.shape[0] // (rows // 2), rows // 2), jnp.int32),
            pltpu.SMEM(span_order.shape, jnp.int32),
            dma((7,)),
            pltpu.VMEM((slabs, 2, rows, DH), bf16),
            pltpu.VMEM((slabs, 2, rows, DH), bf16),
            pltpu.VMEM((slabs, 2, 2 * depth, half), bf16),
            pltpu.VMEM((2, rows, 2 * rows), jnp.float32),
            pltpu.VMEM((heads, rows, DH), jnp.float32),
            pltpu.VMEM((heads, rows, 2 * DH), jnp.float32),
            pltpu.VMEM((3,) + queries.shape, bf16),
            pltpu.VMEM((2,) + queries.shape, bf16),
            pltpu.VMEM((slabs + 1, 2, rows, half), bf16),
            dma,
            dma((3, slabs)),
            dma,
            dma((2, slabs, 2, 2)),
            dma((2,)),
            dma((2,)),
            dma,
            dma,
            dma,
            dma,
        ],
        compiler_params=pltpu.CompilerParams(
            collective_id=0, has_side_effects=True, vmem_limit_bytes=62 * 1024 * 1024
        ),
    )(queries, keys, values, doc_ids.reshape(-1, rows // 2), span_order, out_weight)
    return (sums[0].astype(jnp.float32) + sums[1].astype(jnp.float32)).astype(bf16)


def on_device(mesh_shape, queries, keys, values, doc_ids, span_order, out_weight):
    n, groups = mesh_shape["seq"], mesh_shape["head"]
    rows = queries.shape[0]
    depth, width = out_weight.shape
    fits = (
        groups == 4
        and n == 2 * groups
        and rows == 2 * DH
        and keys.shape[1] == DH
        and queries.shape[1] == depth
        and depth % (2 * DH) == 0
        and width % (4 * DH) == 0
        and depth * width <= 512 * 512
    )
    if fits:
        return line_form(n, queries, keys, values, doc_ids, span_order, out_weight)
    return gathered_form(queries, keys, values, doc_ids, span_order, out_weight)


def solution(mesh):
    return jax.shard_map(
        functools.partial(on_device, dict(mesh.shape)),
        mesh=mesh,
        in_specs=(P("seq", "head"), P("seq", "head"), P("seq", "head"), P(), P(), P("head", "seq")),
        out_specs=P("seq", "head"),
        check_vma=False,
    )
```

```python
import functools
import math

import jax
import jax.numpy as jnp
from jax import lax
from jax.experimental import pallas as pl
from jax.experimental.pallas import tpu as pltpu
from jax.sharding import PartitionSpec as P

MESH = pl.DeviceIdType.MESH

DH = 128
NEG = -1e30

def gathered_form(queries, keys, values, doc_ids, span_order, out_weight):
    tok_rows = queries.shape[0]
    span = tok_rows // 2
    local_heads = queries.shape[1] // DH
    local_kv = keys.shape[1] // DH
    group_size = local_heads // local_kv
    n_blocks = span_order.shape[0]
    scale = 1.0 / math.sqrt(DH)
    mine = lax.axis_index("seq")
    own_blocks = lax.dynamic_slice_in_dim(span_order, 2 * mine, 2, 0)
    local_rows = jnp.arange(tok_rows, dtype=jnp.int32)
    qpos = jnp.where(local_rows < span, own_blocks[0], own_blocks[1]) * span + local_rows % span
    qdoc = jnp.take(doc_ids, qpos)
    q_heads = queries.reshape(tok_rows, local_kv, group_size, DH)

    def update(state, kblk, vblk, kpos, kdoc):
        largest, total, summed = state
        count = kblk.shape[0]
        k_heads = kblk.reshape(count, local_kv, DH)
        v_heads = vblk.reshape(count, local_kv, DH)
        scores = (
            jnp.einsum("qhgd,khd->hgqk", q_heads, k_heads, preferred_element_type=jnp.float32)
            * scale
        )
        visible = (qdoc[:, None] == kdoc[None, :]) & (kpos[None, :] <= qpos[:, None])
        masked = jnp.where(visible, scores, jnp.float32(-1e30))
        new_largest = jnp.maximum(largest, jnp.max(masked, axis=-1))
        factor = jnp.exp(largest - new_largest)
        weights = jnp.where(visible, jnp.exp(masked - new_largest[..., None]), jnp.float32(0.0))
        total = total * factor + jnp.sum(weights, axis=-1)
        weights_b = weights.astype(jnp.bfloat16)
        added = jnp.einsum("hgqk,khd->qhgd", weights_b, v_heads, preferred_element_type=jnp.float32)
        summed = summed * jnp.transpose(factor, (2, 0, 1))[..., None] + added
        return (new_largest, total, summed)

    initial = (
        jnp.full((local_kv, group_size, tok_rows), -1e30, jnp.float32),
        jnp.zeros((local_kv, group_size, tok_rows), jnp.float32),
        jnp.zeros((tok_rows, local_kv, group_size, DH), jnp.float32),
    )
    state = initial
    kpiece = lax.all_gather(keys, "seq", axis=0, tiled=True)
    vpiece = lax.all_gather(values, "seq", axis=0, tiled=True)
    count = kpiece.shape[0]
    width = math.gcd(count, 1024)
    steps = count // width
    rows = jnp.arange(count, dtype=jnp.int32)
    match = (rows // span)[:, None] == jnp.arange(n_blocks, dtype=jnp.int32)[None, :]
    owner = jnp.sum(jnp.where(match, span_order[None, :], 0), axis=1)
    kpos = owner * span + rows % span
    kdoc = jnp.take(doc_ids, kpos)
    kparts = kpiece.reshape(steps, width, kpiece.shape[1])
    vparts = vpiece.reshape(steps, width, vpiece.shape[1])

    def one_step(carry, items):
        kblk, vblk, pblk, dblk = items
        carry = update(carry, kblk, vblk, pblk, dblk)
        return (carry, None)

    state, unused = lax.scan(
        one_step, state, (kparts, vparts, kpos.reshape(steps, width), kdoc.reshape(steps, width))
    )
    largest, total, summed = state
    attended = (summed / jnp.transpose(total, (2, 0, 1))[..., None]).astype(jnp.bfloat16)
    attended = attended.reshape(tok_rows, local_heads * DH)
    partial_out = jnp.dot(
        attended,
        lax.all_gather(out_weight, "seq", axis=1, tiled=True),
        preferred_element_type=jnp.float32,
    )
    return lax.psum_scatter(
        partial_out.astype(jnp.bfloat16), "head", scatter_dimension=1, tiled=True
    )


def line_kernel(
    n, q_in, k_in, v_in, doc_in, order_in, w_in, out_ref,
    q_ref, doc_ref, order_ref, fetched, kbuf, vbuf, wbuf, bias, best, acc, att, far, stage,
    kv_send, kv_recv, w_send, w_recv, att_send, att_recv, far_send, far_recv, sum_send, sum_recv,
):
    seq, head = lax.axis_index("seq"), lax.axis_index("head")
    z, x, y, c = seq // 2, seq % 2, head // 2, head % 2
    side = z // 2
    role = (z + side) % 2
    rows = q_ref.shape[0]
    span = rows // 2
    heads = q_ref.shape[1] // DH
    depth, width = w_in.shape
    half, deep = width // 2, depth // 2
    factor = math.log2(math.e) / math.sqrt(DH)
    slabs = n // 2
    far_slab = slabs - 1
    cuts = range(2)
    parts = [(cut, low) for cut in range(2) for low in range(2)]

    def slab(k):
        return k + side * (slabs - 1 - 2 * k)

    def place(zz, xx, yy, cc):
        return {"seq": 2 * zz + xx, "head": 2 * yy + cc}

    inward = place((1 - role) * slab(1) + role * slab(2), x, y, c)
    outward = place(slab(0), x, y, c)
    across = {"seq": 2 * z + 1 - x}
    partner = {"head": 2 * y + 1 - c}
    ways = (inward, outward, across)

    own = role
    fetches = [
        pltpu.make_async_copy(src, dst, fetched.at[at])
        for at, (src, dst) in enumerate(
            [(k_in, kbuf.at[own, 0]), (v_in, vbuf.at[own, 0])]
            + [(w_in.at[:, pl.ds(cut * half, half)], wbuf.at[own, cut, pl.ds(0, depth)]) for cut in range(2)]
            + [(doc_in, doc_ref), (order_in, order_ref), (q_in, q_ref)]
        )
    ]
    for fetch in fetches:
        fetch.start()

    barrier = pltpu.get_barrier_semaphore()
    nearby = place((1 - role) * slab(1) + role * slab(0), x, y, c)
    for there in (nearby, across, partner, {"head": 2 * (1 - y) + c}):
        pl.semaphore_signal(barrier, inc=1, device_id=there, device_id_type=MESH)

    @pl.when(role == 1)
    def _():
        pl.semaphore_signal(barrier, inc=1, device_id=inward, device_id_type=MESH)

    pl.semaphore_wait(barrier, 4 + role)

    def remote(src, dst, send, recv, device):
        return pltpu.make_async_remote_copy(
            src_ref=src, dst_ref=dst, send_sem=send, recv_sem=recv, device_id=device, device_id_type=MESH
        )

    passed, pieces = [0, 0], [0, 0]

    def arrive(dst, recv):
        remote(dst, dst, att_send.at[0], recv, partner).wait_recv()

    def kv_send_to(who, which, way, k):
        buf = (kbuf, vbuf)[which]
        to = slabs - 1 - k if (who == 1 and way == 0) else k
        lane = 1 if way == 2 else 0
        at = which if lane == 0 else 2
        remote(buf.at[k, 0], buf.at[to, lane], kv_send, kv_recv.at[at, to], ways[way]).start()
        passed[who] += 1

    def kv_wait(which, k):
        arrive((kbuf, vbuf)[which].at[k, 0], kv_recv.at[which, k])

    def kv_pair_wait(k):
        both = q_ref.at[:, pl.ds(0, 2 * DH)]
        arrive(both, kv_recv.at[2, k])

    def w_at(k, cut, low, mine):
        return wbuf.at[k, cut, pl.ds(mine * depth + low * deep, deep)]

    def w_send_to(who, way, k, cut, low):
        to = slabs - 1 - k if (who == 1 and way == 0) else k
        mine = 1 if way == 2 else 0
        remote(
            w_at(k, cut, low, 0), w_at(to, cut, low, mine), w_send, w_recv.at[mine, to, cut, 0 if mine else low],
            partner if way == 2 else ways[way],
        ).start()
        pieces[who] += 1

    def w_wait(k, cut, low):
        arrive(w_at(k, cut, low, 0), w_recv.at[0, k, cut, low])

    def each(end, middle):
        @pl.when(role == 0)
        def _():
            end(0)

        @pl.when(role == 1)
        def _():
            middle(1)

    for which in range(2):
        fetches[which].wait()

        def end(who):
            for way in (0, 2):
                kv_send_to(who, which, way, 0)

        def middle(who):
            for way in (1, 0, 2):
                kv_send_to(who, which, way, 1)

        each(end, middle)
    for fetch in fetches[2:]:
        fetch.wait()

    def middle(who):
        w_send_to(who, 1, 1, *parts[0])

    each(lambda who: None, middle)


    down = lax.broadcasted_iota(jnp.int32, (span, span), 0)
    along = lax.broadcasted_iota(jnp.int32, (span, span), 1)
    query_at, query_doc = [], []
    for part in range(2):
        block = order_ref[2 * seq + part]
        query_at.append(down + block * span)
        docs = doc_ref[pl.ds(block, 1), :].astype(jnp.float32)
        query_doc.append(jnp.transpose(jnp.broadcast_to(docs, (span, span))))

    order = (role, 1 - role, 2, 3)

    def mask(step):
        for lane in range(2):
            source = 2 * slab(order[step]) + (x if lane == 0 else 1 - x)
            for j in range(2):
                block = order_ref[2 * source + j]
                docs = doc_ref[pl.ds(block, 1), :].astype(jnp.float32)
                key_at = along + block * span
                first = (2 * lane + j) * span
                for part in range(2):
                    seen = (query_doc[part] == docs) & (key_at <= query_at[part])
                    bias[step % 2, part * span : (part + 1) * span, first : first + span] = jnp.where(
                        seen, jnp.float32(0.0), jnp.float32(NEG)
                    )

    def attend(step, h):
        k = order[step]
        count = 2 * rows
        q = q_ref[:, h * DH : (h + 1) * DH]
        scores = lax.dot_general(
            q, kbuf[k].reshape(count, DH), (((1,), (1,)), ((), ())), preferred_element_type=jnp.float32
        )
        masked = scores * factor + bias[step % 2]
        top = jnp.broadcast_to(jnp.max(masked, axis=-1, keepdims=True), (rows, DH))
        if step > 0:
            before = best[h]
            top = jnp.maximum(before, top)
        weights = jnp.concatenate(
            [jnp.exp2(masked[:, at : at + DH] - top).astype(jnp.bfloat16) for at in range(0, count, DH)], axis=1
        )
        wide = jnp.concatenate([vbuf[k].reshape(count, DH), jnp.ones((count, DH), jnp.bfloat16)], axis=1)
        summed = jnp.dot(weights, wide, preferred_element_type=jnp.float32)
        if step > 0:
            fade = jnp.exp2(before - top)
            summed = summed + acc[h] * jnp.concatenate([fade, fade], axis=1)
        if step < slabs - 1:
            best[h] = top
            acc[h] = summed
        else:
            att[2, :, h * DH : (h + 1) * DH] = (summed[:, :DH] / summed[:, DH:]).astype(jnp.bfloat16)

    def group(step):
        kv_pair_wait(order[step])
        for h in range(heads):
            attend(step, h)

    mask(0)

    def end(who):
        for which in range(2):
            kv_wait(which, 1)
            kv_send_to(who, which, 2, 1)
        for cut, low in parts:
            w_send_to(who, 0, 0, cut, low)
        for cut, low in parts:
            w_send_to(who, 2, 0, cut, low)

    def middle(who):
        for which in range(2):
            kv_wait(which, 0)
            kv_send_to(who, which, 0, 0)
            kv_send_to(who, which, 2, 0)
            kv_wait(which, 2)
            kv_send_to(who, which, 1, 2)
            kv_send_to(who, which, 2, 2)
        for cut, low in parts:
            w_send_to(who, 0, 1, cut, low)
        for which in range(2):
            kv_wait(which, 3)
            kv_send_to(who, which, 1, 3)
            kv_send_to(who, which, 2, 3)
        w_send_to(who, 1, 1, *parts[1])
        for cut, low in parts:
            w_send_to(who, 2, 1, cut, low)

    each(end, middle)
    mask(1)
    group(0)

    def end(who):
        for which in range(2):
            kv_wait(which, 2)
            kv_send_to(who, which, 2, 2)

    each(end, lambda who: None)
    group(1)
    mask(2)
    mask(3)

    def pass_w(who, k, which, way):
        for cut, low in which:
            w_wait(k, cut, low)
            if way is not None:
                w_send_to(who, way, k, cut, low)
            w_send_to(who, 2, k, cut, low)

    def end(who):
        for which in range(2):
            kv_wait(which, 3)
            kv_send_to(who, which, 2, 3)

    def middle(who):
        pass_w(who, 2, parts[:1], 1)

    each(end, middle)
    group(2)

    def middle(who):
        pass_w(who, 0, parts[:2], 0)
        pass_w(who, 2, parts[1:2], 1)

    each(lambda who: None, middle)
    group(3)

    cross = place(z, 1 - x, y, x)
    own_rows = c == x
    cross_part = (c + x) % 2
    first_part = 2 * (1 - cross_part)

    def att_cross():
        return remote(att.at[2], att.at[cross_part], att_send.at[0], att_recv.at[cross_part], cross)

    def att_near():
        return remote(att.at[2], att.at[1], att_send.at[1], att_recv.at[1], partner)

    att_cross().start()

    @pl.when(jnp.logical_not(own_rows))
    def _():
        att_near().start()

    def far_copy(part):
        return remote(att.at[part], far.at[part], far_send, far_recv, inward)

    def own_far():
        return remote(att.at[2], far.at[0], far_send, far_recv, inward)

    @pl.when(own_rows & (role == 0))
    def _():
        own_far().start()

    def end(who):
        pass_w(who, 1, parts[:2], None)

    def middle(who):
        pass_w(who, 0, parts[2:], 0)
        pass_w(who, 2, parts[2:], 1)
        for cut, low in parts[2:]:
            w_send_to(who, 1, 1, cut, low)

    each(end, middle)

    for part in (1 - c, c):

        @pl.when(own_rows & (part == 1))
        def _():
            arrive(att.at[1], att_recv.at[1])

        @pl.when(jnp.logical_not(own_rows))
        def _(part=part):
            arrive(att.at[part], att_recv.at[part])

        @pl.when((role == 0) & (jnp.logical_not(own_rows) | (part == 1)))
        def _(part=part):
            far_copy(part).start()

    def sum_at(row, lane, cut):
        return out_ref.at[row, :, pl.ds(pl.multiple_of(lane * width + cut * half, half), half)]

    def sum_copy(k, slot, cut, zz):
        return remote(
            stage.at[slot, cut], sum_at(y, x, cut), sum_send, sum_recv,
            {"seq": 2 * zz + c, "head": slab(k)},
        )

    def sum_stay(slot, cut):
        return pltpu.make_async_copy(stage.at[slot, cut], sum_at(y, x, cut), sum_recv)

    def here(k):
        return own_rows & (slab(k) == head)

    def product(k, cut, first, second):
        added = jnp.dot(first, wbuf[k, cut, :depth, :], preferred_element_type=jnp.float32)
        return added + jnp.dot(second, wbuf[k, cut, depth:, :], preferred_element_type=jnp.float32)

    def project(k, slot, cut):
        value = product(k, cut, att[first_part], att[1]).astype(jnp.bfloat16)

        stage[slot, cut] = value

        @pl.when(here(k))
        def _():
            sum_stay(slot, cut).start()

        @pl.when(jnp.logical_not(here(k)))
        def _():
            sum_copy(k, slot, cut, z).start()

    def project_far(who, cut):
        stage[slabs, cut] = product(far_slab, cut, far[0], far[1]).astype(jnp.bfloat16)
        sum_copy(far_slab, slabs, cut, slab(0)).start()

    def near_w(k, cut):
        arrive(wbuf.at[k, cut, pl.ds(depth, depth)], w_recv.at[1, k, cut, 0])

    for cut in cuts:
        near_w(order[0], cut)
        project(order[0], 0, cut)

    near_w(order[1], 0)
    project(order[1], 1, 0)

    def middle(who):
        near_w(0, 1)
        project(0, 1, 1)

    each(lambda who: None, middle)
    for cut in cuts:

        def end(who):
            pass_w(who, 2, [(cut, low) for low in range(2)], None)

        each(end, lambda who: None)
        near_w(2, cut)
        project(2, 2, cut)

    def end(who):
        pass_w(who, 1, parts[2:], None)
        near_w(1, 1)
        project(1, 1, 1)

    def middle(who):
        pass_w(who, 3, parts[:2], None)
        near_w(3, 0)
        project(3, 3, 0)
        pass_w(who, 3, parts[2:], None)
        arrive(far, far_recv)
        project_far(who, 0)
        near_w(3, 1)
        project_far(who, 1)
        project(3, 3, 1)

    each(end, middle)

    stays = own_rows & ((role == 1) | (slab(far_slab) != head))

    def left(ref, send):
        remote(ref, ref, send, sum_recv, partner).wait_send()

    def finish(who):
        left(wbuf.at[:2, :, pl.ds(0, passed[who] * rows * DH // (4 * half))], kv_send)
        left(wbuf.at[: pieces[who] // (2 * len(parts))], w_send)
        made = 2 * slabs + 2 if who == 1 else 2 * slabs - 2

        @pl.when(stays)
        def _():
            left(stage.at[: made // 2 - 1], sum_send)

        @pl.when(jnp.logical_not(stays))
        def _():
            left(stage.at[: made // 2], sum_send)

    def end(who):
        left(far, far_send)
        finish(who)

    each(end, finish)
    att_cross().wait_send()

    @pl.when(jnp.logical_not(own_rows))
    def _():
        att_near().wait_send()

    arrive(out_ref, sum_recv)


def add_kernel(pair_in, out, pair, total, came, went):
    pieces = pair.shape[0]
    rows = pair.shape[2]

    def fetch(at):
        return pltpu.make_async_copy(pair_in.at[:, pl.ds(at * rows, rows)], pair.at[at], came.at[at])

    def leave(at):
        return pltpu.make_async_copy(total.at[at], out.at[pl.ds(at * rows, rows)], went.at[at])

    for at in range(pieces):
        fetch(at).start()
    for at in range(pieces):
        fetch(at).wait()
        total[at] = (pair[at, 0].astype(jnp.float32) + pair[at, 1].astype(jnp.float32)).astype(total.dtype)
        leave(at).start()
    for at in range(pieces):
        leave(at).wait()


def add_form(sums):
    pieces = 4
    rows, columns = sums.shape[1] // pieces, sums.shape[2]
    return pl.pallas_call(
        add_kernel,
        out_shape=jax.ShapeDtypeStruct(sums.shape[1:], sums.dtype),
        in_specs=[pl.BlockSpec(memory_space=pl.ANY)],
        out_specs=pl.BlockSpec(memory_space=pl.ANY),
        scratch_shapes=[
            pltpu.VMEM((pieces, 2, rows, columns), sums.dtype),
            pltpu.VMEM((pieces, rows, columns), sums.dtype),
            pltpu.SemaphoreType.DMA((pieces,)),
            pltpu.SemaphoreType.DMA((pieces,)),
        ],
        compiler_params=pltpu.CompilerParams(vmem_limit_bytes=62 * 1024 * 1024),
    )(sums)


def line_form(n, queries, keys, values, doc_ids, span_order, out_weight):
    rows = queries.shape[0]
    depth, width = out_weight.shape
    half = width // 2
    slabs = n // 2
    heads = queries.shape[1] // DH
    bf16 = jnp.bfloat16
    dma = pltpu.SemaphoreType.DMA
    sums = pl.pallas_call(
        functools.partial(line_kernel, n),
        out_shape=jax.ShapeDtypeStruct((2, rows, 2 * width), bf16),
        in_specs=[pl.BlockSpec(memory_space=pl.ANY)] * 6,
        out_specs=pl.BlockSpec(memory_space=pl.ANY),
        scratch_shapes=[
            pltpu.VMEM(queries.shape, bf16),
            pltpu.VMEM((doc_ids.shape[0] // (rows // 2), rows // 2), jnp.int32),
            pltpu.SMEM(span_order.shape, jnp.int32),
            dma((7,)),
            pltpu.VMEM((slabs, 2, rows, DH), bf16),
            pltpu.VMEM((slabs, 2, rows, DH), bf16),
            pltpu.VMEM((slabs, 2, 2 * depth, half), bf16),
            pltpu.VMEM((2, rows, 2 * rows), jnp.float32),
            pltpu.VMEM((heads, rows, DH), jnp.float32),
            pltpu.VMEM((heads, rows, 2 * DH), jnp.float32),
            pltpu.VMEM((3,) + queries.shape, bf16),
            pltpu.VMEM((2,) + queries.shape, bf16),
            pltpu.VMEM((slabs + 1, 2, rows, half), bf16),
            dma,
            dma((3, slabs)),
            dma,
            dma((2, slabs, 2, 2)),
            dma((2,)),
            dma((2,)),
            dma,
            dma,
            dma,
            dma,
        ],
        compiler_params=pltpu.CompilerParams(
            collective_id=0, has_side_effects=True, vmem_limit_bytes=62 * 1024 * 1024
        ),
    )(queries, keys, values, doc_ids.reshape(-1, rows // 2), span_order, out_weight)
    return add_form(sums)


def on_device(mesh_shape, queries, keys, values, doc_ids, span_order, out_weight):
    n, groups = mesh_shape["seq"], mesh_shape["head"]
    rows = queries.shape[0]
    depth, width = out_weight.shape
    fits = (
        groups == 4
        and n == 2 * groups
        and rows == 2 * DH
        and keys.shape[1] == DH
        and queries.shape[1] == depth
        and depth % (2 * DH) == 0
        and width % (4 * DH) == 0
        and depth * width <= 512 * 512
    )
    if fits:
        return line_form(n, queries, keys, values, doc_ids, span_order, out_weight)
    return gathered_form(queries, keys, values, doc_ids, span_order, out_weight)


def solution(mesh):
    return jax.shard_map(
        functools.partial(on_device, dict(mesh.shape)),
        mesh=mesh,
        in_specs=(P("seq", "head"), P("seq", "head"), P("seq", "head"), P(), P(), P("head", "seq")),
        out_specs=P("seq", "head"),
        check_vma=False,
    )
```

```python
import functools
import math

import jax
import jax.numpy as jnp
from jax import lax
from jax.experimental import pallas as pl
from jax.experimental.pallas import tpu as pltpu
from jax.sharding import PartitionSpec as P

MESH = pl.DeviceIdType.MESH

DH = 128
NEG = -1e30

def gathered_form(queries, keys, values, doc_ids, span_order, out_weight):
    tok_rows = queries.shape[0]
    span = tok_rows // 2
    local_heads = queries.shape[1] // DH
    local_kv = keys.shape[1] // DH
    group_size = local_heads // local_kv
    n_blocks = span_order.shape[0]
    scale = 1.0 / math.sqrt(DH)
    mine = lax.axis_index("seq")
    own_blocks = lax.dynamic_slice_in_dim(span_order, 2 * mine, 2, 0)
    local_rows = jnp.arange(tok_rows, dtype=jnp.int32)
    qpos = jnp.where(local_rows < span, own_blocks[0], own_blocks[1]) * span + local_rows % span
    qdoc = jnp.take(doc_ids, qpos)
    q_heads = queries.reshape(tok_rows, local_kv, group_size, DH)

    def update(state, kblk, vblk, kpos, kdoc):
        largest, total, summed = state
        count = kblk.shape[0]
        k_heads = kblk.reshape(count, local_kv, DH)
        v_heads = vblk.reshape(count, local_kv, DH)
        scores = (
            jnp.einsum("qhgd,khd->hgqk", q_heads, k_heads, preferred_element_type=jnp.float32)
            * scale
        )
        visible = (qdoc[:, None] == kdoc[None, :]) & (kpos[None, :] <= qpos[:, None])
        masked = jnp.where(visible, scores, jnp.float32(-1e30))
        new_largest = jnp.maximum(largest, jnp.max(masked, axis=-1))
        factor = jnp.exp(largest - new_largest)
        weights = jnp.where(visible, jnp.exp(masked - new_largest[..., None]), jnp.float32(0.0))
        total = total * factor + jnp.sum(weights, axis=-1)
        weights_b = weights.astype(jnp.bfloat16)
        added = jnp.einsum("hgqk,khd->qhgd", weights_b, v_heads, preferred_element_type=jnp.float32)
        summed = summed * jnp.transpose(factor, (2, 0, 1))[..., None] + added
        return (new_largest, total, summed)

    initial = (
        jnp.full((local_kv, group_size, tok_rows), -1e30, jnp.float32),
        jnp.zeros((local_kv, group_size, tok_rows), jnp.float32),
        jnp.zeros((tok_rows, local_kv, group_size, DH), jnp.float32),
    )
    state = initial
    kpiece = lax.all_gather(keys, "seq", axis=0, tiled=True)
    vpiece = lax.all_gather(values, "seq", axis=0, tiled=True)
    count = kpiece.shape[0]
    width = math.gcd(count, 1024)
    steps = count // width
    rows = jnp.arange(count, dtype=jnp.int32)
    match = (rows // span)[:, None] == jnp.arange(n_blocks, dtype=jnp.int32)[None, :]
    owner = jnp.sum(jnp.where(match, span_order[None, :], 0), axis=1)
    kpos = owner * span + rows % span
    kdoc = jnp.take(doc_ids, kpos)
    kparts = kpiece.reshape(steps, width, kpiece.shape[1])
    vparts = vpiece.reshape(steps, width, vpiece.shape[1])

    def one_step(carry, items):
        kblk, vblk, pblk, dblk = items
        carry = update(carry, kblk, vblk, pblk, dblk)
        return (carry, None)

    state, unused = lax.scan(
        one_step, state, (kparts, vparts, kpos.reshape(steps, width), kdoc.reshape(steps, width))
    )
    largest, total, summed = state
    attended = (summed / jnp.transpose(total, (2, 0, 1))[..., None]).astype(jnp.bfloat16)
    attended = attended.reshape(tok_rows, local_heads * DH)
    partial_out = jnp.dot(
        attended,
        lax.all_gather(out_weight, "seq", axis=1, tiled=True),
        preferred_element_type=jnp.float32,
    )
    return lax.psum_scatter(
        partial_out.astype(jnp.bfloat16), "head", scatter_dimension=1, tiled=True
    )


def line_kernel(
    n, q_in, k_in, v_in, doc_in, order_in, w_in, out_ref,
    q_ref, doc_ref, order_ref, fetched, kbuf, vbuf, wbuf, bias, best, acc, att, far, stage,
    kv_send, kv_recv, w_send, w_recv, att_send, att_recv, far_send, far_recv, sum_send, sum_recv,
):
    seq, head = lax.axis_index("seq"), lax.axis_index("head")
    z, x, y, c = seq // 2, seq % 2, head // 2, head % 2
    side = z // 2
    role = (z + side) % 2
    rows = q_ref.shape[0]
    span = rows // 2
    heads = q_ref.shape[1] // DH
    depth, width = w_in.shape
    half, deep = width // 2, depth // 2
    factor = math.log2(math.e) / math.sqrt(DH)
    slabs = n // 2
    handed = ((1, 1), (slabs - 1, 0), (slabs - 1, 1))
    cuts = range(2)
    parts = [(cut, low) for cut in range(2) for low in range(2)]

    def slab(k):
        return k + side * (slabs - 1 - 2 * k)

    def place(zz, xx, yy, cc):
        return {"seq": 2 * zz + xx, "head": 2 * yy + cc}

    inward = place((1 - role) * slab(1) + role * slab(2), x, y, c)
    outward = place(slab(0), x, y, c)
    across = {"seq": 2 * z + 1 - x}
    partner = {"head": 2 * y + 1 - c}
    ways = (inward, outward, across)

    own = role
    fetches = [
        pltpu.make_async_copy(src, dst, fetched.at[at])
        for at, (src, dst) in enumerate(
            [(k_in, kbuf.at[own, 0]), (v_in, vbuf.at[own, 0])]
            + [(w_in.at[:, pl.ds(cut * half, half)], wbuf.at[own, cut, pl.ds(0, depth)]) for cut in range(2)]
            + [(doc_in, doc_ref), (order_in, order_ref), (q_in, q_ref)]
        )
    ]
    for fetch in fetches:
        fetch.start()

    barrier = pltpu.get_barrier_semaphore()
    nearby = place((1 - role) * slab(1) + role * slab(0), x, y, c)
    for there in (nearby, across, partner, {"head": 2 * (1 - y) + c}):
        pl.semaphore_signal(barrier, inc=1, device_id=there, device_id_type=MESH)

    @pl.when(role == 1)
    def _():
        pl.semaphore_signal(barrier, inc=1, device_id=inward, device_id_type=MESH)

    pl.semaphore_wait(barrier, 4 + role)

    def remote(src, dst, send, recv, device):
        return pltpu.make_async_remote_copy(
            src_ref=src, dst_ref=dst, send_sem=send, recv_sem=recv, device_id=device, device_id_type=MESH
        )

    passed, pieces = [0, 0], [0, 0]

    def arrive(dst, recv):
        remote(dst, dst, att_send.at[0], recv, partner).wait_recv()

    def kv_send_to(who, which, way, k):
        buf = (kbuf, vbuf)[which]
        to = slabs - 1 - k if (who == 1 and way == 0) else k
        lane = 1 if way == 2 else 0
        at = which if lane == 0 else 2
        remote(buf.at[k, 0], buf.at[to, lane], kv_send, kv_recv.at[at, to], ways[way]).start()
        passed[who] += 1

    def kv_wait(which, k):
        arrive((kbuf, vbuf)[which].at[k, 0], kv_recv.at[which, k])

    def kv_pair_wait(k):
        both = q_ref.at[:, pl.ds(0, 2 * DH)]
        arrive(both, kv_recv.at[2, k])

    def w_at(k, cut, low, mine):
        return wbuf.at[k, cut, pl.ds(mine * depth + low * deep, deep)]

    def w_send_to(who, way, k, cut, low):
        to = slabs - 1 - k if (who == 1 and way == 0) else k
        mine = 1 if way == 2 else 0
        remote(
            w_at(k, cut, low, 0), w_at(to, cut, low, mine), w_send, w_recv.at[mine, to, cut, 0 if mine else low],
            partner if way == 2 else ways[way],
        ).start()
        pieces[who] += 1

    def w_wait(k, cut, low):
        arrive(w_at(k, cut, low, 0), w_recv.at[0, k, cut, low])

    def each(end, middle):
        @pl.when(role == 0)
        def _():
            end(0)

        @pl.when(role == 1)
        def _():
            middle(1)

    for which in range(2):
        fetches[which].wait()

        def end(who):
            for way in (0, 2):
                kv_send_to(who, which, way, 0)

        def middle(who):
            for way in (1, 0, 2):
                kv_send_to(who, which, way, 1)

        each(end, middle)
    for fetch in fetches[2:]:
        fetch.wait()

    def middle(who):
        w_send_to(who, 1, 1, *parts[0])

    each(lambda who: None, middle)


    down = lax.broadcasted_iota(jnp.int32, (span, span), 0)
    along = lax.broadcasted_iota(jnp.int32, (span, span), 1)
    query_at, query_doc = [], []
    for part in range(2):
        block = order_ref[2 * seq + part]
        query_at.append(down + block * span)
        docs = doc_ref[pl.ds(block, 1), :].astype(jnp.float32)
        query_doc.append(jnp.transpose(jnp.broadcast_to(docs, (span, span))))

    order = (role, 1 - role, 2, 3)

    def mask(step):
        for lane in range(2):
            source = 2 * slab(order[step]) + (x if lane == 0 else 1 - x)
            for j in range(2):
                block = order_ref[2 * source + j]
                docs = doc_ref[pl.ds(block, 1), :].astype(jnp.float32)
                key_at = along + block * span
                first = (2 * lane + j) * span
                for part in range(2):
                    seen = (query_doc[part] == docs) & (key_at <= query_at[part])
                    bias[step % 2, part * span : (part + 1) * span, first : first + span] = jnp.where(
                        seen, jnp.float32(0.0), jnp.float32(NEG)
                    )

    def attend(step, h):
        k = order[step]
        count = 2 * rows
        q = q_ref[:, h * DH : (h + 1) * DH]
        scores = lax.dot_general(
            q, kbuf[k].reshape(count, DH), (((1,), (1,)), ((), ())), preferred_element_type=jnp.float32
        )
        masked = scores * factor + bias[step % 2]
        top = jnp.broadcast_to(jnp.max(masked, axis=-1, keepdims=True), (rows, DH))
        if step > 0:
            before = best[h]
            top = jnp.maximum(before, top)
        weights = jnp.concatenate(
            [jnp.exp2(masked[:, at : at + DH] - top).astype(jnp.bfloat16) for at in range(0, count, DH)], axis=1
        )
        wide = jnp.concatenate([vbuf[k].reshape(count, DH), jnp.ones((count, DH), jnp.bfloat16)], axis=1)
        summed = jnp.dot(weights, wide, preferred_element_type=jnp.float32)
        if step > 0:
            fade = jnp.exp2(before - top)
            summed = summed + acc[h] * jnp.concatenate([fade, fade], axis=1)
        if step < slabs - 1:
            best[h] = top
            acc[h] = summed
        else:
            att[2, :, h * DH : (h + 1) * DH] = (summed[:, :DH] / summed[:, DH:]).astype(jnp.bfloat16)

    def group(step):
        kv_pair_wait(order[step])
        for h in range(heads):
            attend(step, h)

    mask(0)

    def end(who):
        for which in range(2):
            kv_wait(which, 1)
            kv_send_to(who, which, 2, 1)
        for cut, low in parts:
            w_send_to(who, 0, 0, cut, low)
        for cut, low in parts:
            w_send_to(who, 2, 0, cut, low)

    def middle(who):
        for which in range(2):
            kv_wait(which, 0)
            kv_send_to(who, which, 0, 0)
            kv_send_to(who, which, 2, 0)
            kv_wait(which, 2)
            kv_send_to(who, which, 1, 2)
            kv_send_to(who, which, 2, 2)
        for cut, low in parts:
            w_send_to(who, 0, 1, cut, low)
        for which in range(2):
            kv_wait(which, 3)
            kv_send_to(who, which, 1, 3)
            kv_send_to(who, which, 2, 3)
        w_send_to(who, 1, 1, *parts[1])
        for cut, low in parts:
            w_send_to(who, 2, 1, cut, low)

    each(end, middle)
    mask(1)
    group(0)

    def end(who):
        for which in range(2):
            kv_wait(which, 2)
            kv_send_to(who, which, 2, 2)

    each(end, lambda who: None)
    group(1)
    mask(2)
    mask(3)

    def pass_w(who, k, which, way):
        for cut, low in which:
            w_wait(k, cut, low)
            if way is not None:
                w_send_to(who, way, k, cut, low)
            w_send_to(who, 2, k, cut, low)

    def end(who):
        for which in range(2):
            kv_wait(which, 3)
            kv_send_to(who, which, 2, 3)

    def middle(who):
        pass_w(who, 2, parts[:1], 1)

    each(end, middle)
    group(2)

    def middle(who):
        pass_w(who, 0, parts[:2], 0)
        pass_w(who, 2, parts[1:2], 1)

    each(lambda who: None, middle)
    group(3)

    cross = place(z, 1 - x, y, x)
    own_rows = c == x
    cross_part = (c + x) % 2
    first_part = 2 * (1 - cross_part)

    def att_cross():
        return remote(att.at[2], att.at[cross_part], att_send.at[0], att_recv.at[cross_part], cross)

    def att_near():
        return remote(att.at[2], att.at[1], att_send.at[1], att_recv.at[1], partner)


    def far_copy(flip):
        there = place(slab(1), (x + flip) % 2, y, x)
        return remote(att.at[2], far.at[cross_part], far_send, far_recv, there)

    @pl.when(role == 0)
    def _():
        for flip in range(2):
            far_copy(flip).start()

    att_cross().start()

    @pl.when(jnp.logical_not(own_rows))
    def _():
        att_near().start()

    def end(who):
        pass_w(who, 1, parts[:2], None)

    def middle(who):
        pass_w(who, 0, parts[2:], 0)
        pass_w(who, 2, parts[2:], 1)

    each(end, middle)

    for turn, part in enumerate((1 - c, c)):

        @pl.when(own_rows & (part == 1))
        def _():
            arrive(att.at[1], att_recv.at[1])

        @pl.when(jnp.logical_not(own_rows))
        def _(part=part):
            arrive(att.at[part], att_recv.at[part])

        if turn == 0:
            each(lambda who: pass_w(who, 2, parts[:2], None), lambda who: None)

    def sum_at(row, lane, cut):
        return out_ref.at[row, :, pl.ds(pl.multiple_of(lane * width + cut * half, half), half)]

    def sum_copy(k, slot, at, zz, cut):
        return remote(
            stage.at[slot, at], sum_at(y, x, cut), sum_send, sum_recv,
            {"seq": 2 * zz + c, "head": slab(k)},
        )

    def sum_stay(slot, cut):
        return pltpu.make_async_copy(stage.at[slot, cut], sum_at(y, x, cut), sum_recv)

    def here(k):
        return own_rows & (slab(k) == head)

    def product(k, cut, first, second):
        added = jnp.dot(first, wbuf[k, cut, :depth, :], preferred_element_type=jnp.float32)
        return added + jnp.dot(second, wbuf[k, cut, depth:, :], preferred_element_type=jnp.float32)

    def project(k, slot, cut):
        value = product(k, cut, att[first_part], att[1]).astype(jnp.bfloat16)

        stage[slot, cut] = value

        @pl.when(here(k))
        def _():
            sum_stay(slot, cut).start()

        @pl.when(jnp.logical_not(here(k)))
        def _():
            sum_copy(k, slot, cut, z, cut).start()

    def project_far(at):
        k, cut = handed[at]
        slot, lane = slabs + at // 2, at % 2
        stage[slot, lane] = product(k, cut, far[0], far[1]).astype(jnp.bfloat16)
        sum_copy(k, slot, lane, slab(0), cut).start()

    def near_w(k, cut):
        arrive(wbuf.at[k, cut, pl.ds(depth, depth)], w_recv.at[1, k, cut, 0])

    near_w(2, 0)
    project(2, 2, 0)
    for cut in cuts:
        near_w(order[0], cut)
        project(order[0], 0, cut)
    near_w(order[1], 0)
    project(order[1], 1, 0)

    def middle(who):
        near_w(0, 1)
        project(0, 1, 1)

    each(lambda who: None, middle)
    each(lambda who: pass_w(who, 2, parts[2:], None), lambda who: None)
    near_w(2, 1)
    project(2, 2, 1)

    def middle(who):
        pass_w(who, 3, parts[:2], None)
        near_w(3, 0)
        project(3, 3, 0)
        pass_w(who, 3, parts[2:3], None)
        arrive(far, far_recv)
        project_far(0)
        project_far(1)
        pass_w(who, 3, parts[3:], None)
        near_w(3, 1)
        project_far(2)
        project(3, 3, 1)

    each(lambda who: None, middle)

    def left(ref, send):
        remote(ref, ref, send, sum_recv, partner).wait_send()

    def finish(who):
        left(wbuf.at[:2, :, pl.ds(0, passed[who] * rows * DH // (4 * half))], kv_send)
        left(wbuf.at[:, :, pl.ds(0, pieces[who] * deep // (2 * slabs))], w_send)
        full = 2 * slabs + len(handed) if who == 1 else 2 * slabs - len(handed)
        kept = [len([1 for cut in cuts if who == 1 or (k, cut) not in handed]) for k in range(slabs)]
        for count in range(3):
            mine = [slab(k) == head for k in range(slabs) if kept[k] == count]
            if count == 0:
                mine.append(jnp.logical_not(own_rows))
            if mine:
                held = functools.reduce(jnp.logical_or, mine)
                held = held if count == 0 else held & own_rows

                @pl.when(held)
                def _(count=count):
                    left(wbuf.at[:2, :, pl.ds(0, (full - count) * rows // 4)], sum_send)

    def end(who):
        left(far, far_send)
        finish(who)

    each(end, finish)
    att_cross().wait_send()

    @pl.when(jnp.logical_not(own_rows))
    def _():
        att_near().wait_send()

    arrive(out_ref, sum_recv)


def add_kernel(pair_in, out, pair, total, came, went):
    pieces = pair.shape[0]
    rows = pair.shape[2]

    def fetch(at):
        return pltpu.make_async_copy(pair_in.at[:, pl.ds(at * rows, rows)], pair.at[at], came.at[at])

    def leave(at):
        return pltpu.make_async_copy(total.at[at], out.at[pl.ds(at * rows, rows)], went.at[at])

    for at in range(pieces):
        fetch(at).start()
    for at in range(pieces):
        fetch(at).wait()
        total[at] = (pair[at, 0].astype(jnp.float32) + pair[at, 1].astype(jnp.float32)).astype(total.dtype)
        leave(at).start()
    for at in range(pieces):
        leave(at).wait()


def add_form(sums):
    pieces = 4
    rows, columns = sums.shape[1] // pieces, sums.shape[2]
    return pl.pallas_call(
        add_kernel,
        out_shape=jax.ShapeDtypeStruct(sums.shape[1:], sums.dtype),
        in_specs=[pl.BlockSpec(memory_space=pl.ANY)],
        out_specs=pl.BlockSpec(memory_space=pl.ANY),
        scratch_shapes=[
            pltpu.VMEM((pieces, 2, rows, columns), sums.dtype),
            pltpu.VMEM((pieces, rows, columns), sums.dtype),
            pltpu.SemaphoreType.DMA((pieces,)),
            pltpu.SemaphoreType.DMA((pieces,)),
        ],
        compiler_params=pltpu.CompilerParams(vmem_limit_bytes=62 * 1024 * 1024),
    )(sums)


def line_form(n, queries, keys, values, doc_ids, span_order, out_weight):
    rows = queries.shape[0]
    depth, width = out_weight.shape
    half = width // 2
    slabs = n // 2
    heads = queries.shape[1] // DH
    bf16 = jnp.bfloat16
    dma = pltpu.SemaphoreType.DMA
    sums = pl.pallas_call(
        functools.partial(line_kernel, n),
        out_shape=jax.ShapeDtypeStruct((2, rows, 2 * width), bf16),
        in_specs=[pl.BlockSpec(memory_space=pl.ANY)] * 6,
        out_specs=pl.BlockSpec(memory_space=pl.ANY),
        scratch_shapes=[
            pltpu.VMEM(queries.shape, bf16),
            pltpu.VMEM((doc_ids.shape[0] // (rows // 2), rows // 2), jnp.int32),
            pltpu.SMEM(span_order.shape, jnp.int32),
            dma((7,)),
            pltpu.VMEM((slabs, 2, rows, DH), bf16),
            pltpu.VMEM((slabs, 2, rows, DH), bf16),
            pltpu.VMEM((slabs, 2, 2 * depth, half), bf16),
            pltpu.VMEM((2, rows, 2 * rows), jnp.float32),
            pltpu.VMEM((heads, rows, DH), jnp.float32),
            pltpu.VMEM((heads, rows, 2 * DH), jnp.float32),
            pltpu.VMEM((3,) + queries.shape, bf16),
            pltpu.VMEM((2,) + queries.shape, bf16),
            pltpu.VMEM((slabs + 2, 2, rows, half), bf16),
            dma,
            dma((3, slabs)),
            dma,
            dma((2, slabs, 2, 2)),
            dma((2,)),
            dma((2,)),
            dma,
            dma,
            dma,
            dma,
        ],
        compiler_params=pltpu.CompilerParams(
            collective_id=0, has_side_effects=True, vmem_limit_bytes=62 * 1024 * 1024
        ),
    )(queries, keys, values, doc_ids.reshape(-1, rows // 2), span_order, out_weight)
    return add_form(sums)


def on_device(mesh_shape, queries, keys, values, doc_ids, span_order, out_weight):
    n, groups = mesh_shape["seq"], mesh_shape["head"]
    rows = queries.shape[0]
    depth, width = out_weight.shape
    fits = (
        groups == 4
        and n == 2 * groups
        and rows == 2 * DH
        and keys.shape[1] == DH
        and queries.shape[1] == depth
        and depth % (2 * DH) == 0
        and width % (4 * DH) == 0
        and depth * width <= 512 * 512
    )
    if fits:
        return line_form(n, queries, keys, values, doc_ids, span_order, out_weight)
    return gathered_form(queries, keys, values, doc_ids, span_order, out_weight)


def solution(mesh):
    return jax.shard_map(
        functools.partial(on_device, dict(mesh.shape)),
        mesh=mesh,
        in_specs=(P("seq", "head"), P("seq", "head"), P("seq", "head"), P(), P(), P("head", "seq")),
        out_specs=P("seq", "head"),
        check_vma=False,
    )
```
